256 devices in a mesh: seq: 64 (over x, z, core), head: 4 (over y).
Axes of the slice: x: 4, y: 4, z: 8, core: 2. Of those that a mesh axis runs over, the one named last changes fastest.
Arguments:
- queries: bfloat16 [65536, 1536], P('seq', 'head'), may hold values from -5 to 5
- key_vectors: bfloat16 [65536, 1536], P('seq', 'head'), may hold values from -5 to 5
- value_vectors: bfloat16 [65536, 1536], P('seq', 'head'), may hold values from -6 to 6
- out_grad: bfloat16 [65536, 1536], P('seq', 'head'), may hold values from -6 to 6
- gate_logit: float32 [12], P('head'), may hold values from -2 to 2
- doc_index: int32 [64], replicated, may hold values from 0 to 3, never falling along the last dimension, each value on 1 to 32 neighbouring positions
Outputs:
- query_grad: float32 [65536, 1536], P('seq', 'head')
- key_grad: float32 [65536, 1536], P('seq', 'head')
- value_grad: float32 [65536, 1536], P('seq', 'head')
- gate_grad: float32 [12], P('head')
The draws below stay inside these ranges and needn't reach their ends.
Inputs may be any that keep to these rules, and one draw needn't show every extreme that they name: `doc_index`: never falls from one segment to the next; every document holds 1 to 32 segments, and one holds exactly 32.
All inputs are finite; a program needn't handle non-finite values.
Results may differ from the reference program's by a relative error of at most 0.0017.
The reference program's roundings to bfloat16 on the way (of `attention_low` and `score_grad`) count: a program that leaves them out, or rounds other values in their place, can miss the bound.
Values sent between devices are 32-bit elements; how exact they have to be, the bound alone decides.
A program may use at most 128 MiB of HBM per device.

```python
import math
import jax
import jax.numpy as jnp
import numpy as np
from jax import lax

H = 12
HD = 128
TOK_DEV = 1024
DOCS = 4
SHARDS = 64
TOKENS = 65536


def paired(base_key):
    grid_shape = (TOKENS, H * HD)
    first_key, second_key, scale_key, other_scale, sign_key, noise_key = jax.random.split(base_key, 6)
    query_draw = jax.random.truncated_normal(first_key, -5.0, 5.0, grid_shape, jnp.float32)
    key_draw = jax.random.truncated_normal(second_key, -5.0, 5.0, grid_shape, jnp.float32)
    noise = jax.random.normal(noise_key, grid_shape, jnp.float32)
    value_draw = jnp.clip(1.8 * key_draw + 0.6 * noise, -6.0, 6.0)
    return (query_draw, key_draw, value_draw)


def draw_queries(key, part):
    return paired(jax.random.fold_in(key, 11))[0].astype(jnp.bfloat16)


def draw_key_vectors(key, part):
    return paired(jax.random.fold_in(key, 11))[1].astype(jnp.bfloat16)


def draw_value_vectors(key, part):
    return paired(jax.random.fold_in(key, 11))[2].astype(jnp.bfloat16)


def level_of(own_key, shape, pieces, least, largest):
    factor_of, own = 1.0, jax.random.fold_in(own_key, 6)
    for axis_at, parts in pieces:
        draws = jnp.exp(jax.random.uniform(jax.random.fold_in(own, axis_at), (parts,), jnp.float32, least / len(pieces), largest / len(pieces)))
        factor_of = factor_of * jnp.repeat(draws, shape[axis_at] // parts).reshape([-1 if axis == axis_at else 1 for axis in range(len(shape))])
    return factor_of


def profile(number_of, total, bound, slope):
    loads = [(1 << 20) // math.isqrt(standing ** slope) + 1 for standing in range(2, number_of + 1)]
    rest, given = total - bound - (number_of - 1), [1] * (number_of - 1)
    while rest > 0:
        free = [i for i in range(number_of - 1) if given[i] < bound]
        pool, remaining = sum([loads[i] for i in free]), rest
        for i in free:
            more = min(bound - given[i], max(1, remaining * loads[i] // pool), rest)
            given[i] = given[i] + more
            rest = rest - more
    return np.array([bound] + given)


def ragged(stream_key, amount, total, bound, lean):
    if amount == 2:
        one = jax.random.randint(stream_key, (), max(1, total - bound), min(bound, total - 1) + 1)
        return jnp.stack([one, total - one])
    sizes = jnp.asarray(profile(amount, total, bound, lean), jnp.int32)
    couples = (amount - 1) // 2
    giver, sink = sizes[1:1 + 2 * couples:2], sizes[2:2 + 2 * couples:2]
    slack = jnp.minimum(giver - 1, bound - sink)
    passed = jax.random.randint(jax.random.fold_in(stream_key, 1), (couples,), 0, 1 << 20) % (slack + 1)
    sizes = sizes.at[1:1 + 2 * couples:2].set(giver - passed).at[2:2 + 2 * couples:2].set(sink + passed)
    return sizes[jax.random.permutation(jax.random.fold_in(stream_key, 2), amount)]


def centred(rng, dims, deviation, reach, cuts=(), held_as=jnp.bfloat16):
    result = deviation * jax.random.normal(rng, dims, jnp.float32)
    if cuts:
        result = result * level_of(rng, dims, cuts, -0.22, 0.18)
    return jnp.clip(result, -reach, reach).astype(held_as)


def setup_inputs(seed: int = 0) -> dict:
    seeds = jax.random.split(jax.random.key(seed), 7)
    return {
        "queries": draw_queries(jax.random.fold_in(seeds[6], 71), 0),
        "key_vectors": draw_key_vectors(jax.random.fold_in(seeds[6], 71), 0),
        "value_vectors": draw_value_vectors(jax.random.fold_in(seeds[6], 71), 0),
        "out_grad": centred(seeds[3], (TOKENS, H * HD), 1.0, 6.0, ((0, 64), (1, 4))),
        "gate_logit": jnp.clip(jax.random.uniform(seeds[4], (H,), jnp.float32, -2.0, 2.0) * level_of(seeds[4], (H,), ((0, 4),), -0.4, 0.0), -2.0, 2.0),
        "doc_index": jnp.searchsorted(jnp.cumsum(ragged(seeds[5], DOCS, SHARDS, SHARDS // 2, 2)), jnp.arange(SHARDS), side="right").astype(jnp.int32),
    }


def feature(values_in):
    return jnp.where(values_in > 0, values_in + 1.0, jnp.exp(jnp.minimum(values_in, 0.0)))


def feature_slope(values_in):
    return jnp.where(values_in > 0, 1.0, jnp.exp(jnp.minimum(values_in, 0.0)))


def contribution(key_vectors, value_vectors, head_count):
    row_count = key_vectors.shape[0]
    key_feature = feature(key_vectors.astype(jnp.float32)).astype(jnp.bfloat16)
    feature_three = key_feature.reshape(row_count, head_count, -1).astype(jnp.float32)
    value_three = value_vectors.reshape(row_count, head_count, -1).astype(jnp.float32)
    memory_part = jnp.einsum("nhd,nhe->hde", feature_three, value_three, precision=lax.Precision.HIGHEST)
    norm_part = jnp.sum(feature_three, axis=0)
    return memory_part, norm_part, key_feature


def head_work(head_index, queries, key_vectors, value_vectors, out_grad, query_feature, memory_prev, norm_prev, gate_prob):
    head_size = memory_prev.shape[-1]
    row_count = queries.shape[0]

    def take_columns(matrix):
        return lax.dynamic_slice_in_dim(matrix, head_index * head_size, head_size, 1)

    query_head = take_columns(queries)
    key_head = take_columns(key_vectors)
    value_head = take_columns(value_vectors)
    grad_head = take_columns(out_grad)
    query_float = take_columns(query_feature).astype(jnp.float32)
    memory_share = gate_prob[head_index]
    local_share = 1.0 - memory_share
    score_scale = head_size ** -0.5
    scores = lax.dot_general(query_head, key_head, (((1,), (1,)), ((), ())), preferred_element_type=jnp.float32) * score_scale
    row_ids = lax.broadcasted_iota(jnp.int32, (row_count, row_count), 0)
    col_ids = lax.broadcasted_iota(jnp.int32, (row_count, row_count), 1)
    scores = jnp.where(row_ids >= col_ids, scores, -1e30)
    attention = jnp.exp(scores - jnp.max(scores, axis=1, keepdims=True))
    attention = attention / jnp.sum(attention, axis=1, keepdims=True)
    attention_low = attention.astype(jnp.bfloat16)
    local_read = jnp.dot(attention_low, value_head, preferred_element_type=jnp.float32)
    prob_grad = local_share * lax.dot_general(grad_head, value_head, (((1,), (1,)), ((), ())), preferred_element_type=jnp.float32)
    row_delta = jnp.sum(prob_grad * attention, axis=1, keepdims=True)
    score_grad = (attention * (prob_grad - row_delta)).astype(jnp.bfloat16)
    query_local = jnp.dot(score_grad, key_head, preferred_element_type=jnp.float32) * score_scale
    key_local = lax.dot_general(score_grad, query_head, (((0,), (0,)), ((), ())), preferred_element_type=jnp.float32) * score_scale
    value_local = local_share * lax.dot_general(attention_low, grad_head, (((0,), (0,)), ((), ())), preferred_element_type=jnp.float32)
    memory_head = memory_prev[head_index]
    norm_head = norm_prev[head_index]
    numerator = jnp.dot(query_float, memory_head, precision=lax.Precision.HIGHEST)
    denominator = 1.0 + jnp.dot(query_float, norm_head, precision=lax.Precision.HIGHEST)
    memory_read = numerator / denominator[:, None]
    grad_float = grad_head.astype(jnp.float32)
    num_grad = memory_share * grad_float / denominator[:, None]
    den_grad = -memory_share * jnp.sum(grad_float * memory_read, axis=1) / denominator
    grad_memory = lax.dot_general(query_float, num_grad, (((0,), (0,)), ((), ())), precision=lax.Precision.HIGHEST)
    grad_norm = jnp.dot(den_grad, query_float, precision=lax.Precision.HIGHEST)
    feature_grad = lax.dot_general(num_grad, memory_head, (((1,), (1,)), ((), ())), precision=lax.Precision.HIGHEST) + den_grad[:, None] * norm_head[None, :]
    query_grad = query_local + feature_grad * feature_slope(query_head.astype(jnp.float32))
    gate_part = memory_share * local_share * jnp.sum(grad_float * (memory_read - local_read))
    return query_grad, key_local, value_local, grad_memory, grad_norm, gate_part


def to_rows(stacked):
    return jnp.transpose(stacked, (1, 0, 2)).reshape(stacked.shape[1], -1)


def shard_work(queries, key_vectors, value_vectors, out_grad, memory_prev, norm_prev, gate_prob):
    query_feature = feature(queries.astype(jnp.float32)).astype(jnp.bfloat16)

    def one_head(head_index):
        return head_work(head_index, queries, key_vectors, value_vectors, out_grad, query_feature, memory_prev, norm_prev, gate_prob)

    results = lax.map(one_head, jnp.arange(gate_prob.shape[0], dtype=jnp.int32))
    return to_rows(results[0]), to_rows(results[1]), to_rows(results[2]), results[3], results[4], results[5]


def finish(key_vectors, value_vectors, key_feature, key_local, value_local, later_memory, later_norm):
    row_count = key_vectors.shape[0]
    head_count = later_memory.shape[0]
    value_three = value_vectors.reshape(row_count, head_count, -1).astype(jnp.float32)
    feature_three = key_feature.reshape(row_count, head_count, -1).astype(jnp.float32)
    key_three = key_vectors.reshape(row_count, head_count, -1).astype(jnp.float32)
    feature_grad = jnp.einsum("nhe,hde->nhd", value_three, later_memory, precision=lax.Precision.HIGHEST) + later_norm[None]
    key_grad = key_local + (feature_grad * feature_slope(key_three)).reshape(row_count, -1)
    value_extra = jnp.einsum("nhd,hde->nhe", feature_three, later_memory, precision=lax.Precision.HIGHEST)
    value_grad = value_local + value_extra.reshape(row_count, -1)
    return key_grad, value_grad


def reference(queries, key_vectors, value_vectors, out_grad, gate_logit, doc_index):
    width = H * HD

    def by_shard(matrix):
        return matrix.reshape(SHARDS, TOK_DEV, width)

    query_shards = by_shard(queries)
    key_shards = by_shard(key_vectors)
    value_shards = by_shard(value_vectors)
    grad_shards = by_shard(out_grad)
    gate_prob = jax.nn.sigmoid(gate_logit)
    memory_part, norm_part, key_feature = lax.map(lambda packed: contribution(packed[0], packed[1], H), (key_shards, value_shards))
    opening = jnp.concatenate([jnp.ones((1,), jnp.bool_), doc_index[1:] != doc_index[:-1]])
    closing = jnp.concatenate([doc_index[:-1] != doc_index[1:], jnp.ones((1,), jnp.bool_)])
    start_state = (jnp.zeros((H, HD, HD), jnp.float32), jnp.zeros((H, HD), jnp.float32))

    def forward_step(totals, packed):
        memory_before = jnp.where(packed[2], 0.0, totals[0])
        norm_before = jnp.where(packed[2], 0.0, totals[1])
        return (memory_before + packed[0], norm_before + packed[1]), (memory_before, norm_before)

    final_state, prev_state = lax.scan(forward_step, start_state, (memory_part, norm_part, opening))
    memory_prev, norm_prev = prev_state

    def run_shard(packed):
        return shard_work(packed[0], packed[1], packed[2], packed[3], packed[4], packed[5], gate_prob)

    query_grad, key_local, value_local, grad_memory, grad_norm, gate_parts = lax.map(run_shard, (query_shards, key_shards, value_shards, grad_shards, memory_prev, norm_prev))

    def backward_step(totals, packed):
        memory_after = jnp.where(packed[2], 0.0, totals[0])
        norm_after = jnp.where(packed[2], 0.0, totals[1])
        return (memory_after + packed[0], norm_after + packed[1]), (memory_after, norm_after)

    back_state, later_state = lax.scan(backward_step, start_state, (grad_memory, grad_norm, closing), reverse=True)
    later_memory, later_norm = later_state

    def run_finish(packed):
        return finish(packed[0], packed[1], packed[2], packed[3], packed[4], packed[5], packed[6])

    key_grad, value_grad = lax.map(run_finish, (key_shards, value_shards, key_feature, key_local, value_local, later_memory, later_norm))
    gate_grad = jnp.sum(gate_parts, axis=0)
    return query_grad.reshape(TOKENS, width), key_grad.reshape(TOKENS, width), value_grad.reshape(TOKENS, width), gate_grad
```

```python
import functools
import math

import jax
import jax.numpy as jnp
from jax import lax
from jax.experimental import pallas as pl
from jax.experimental.pallas import tpu as pltpu
from jax.sharding import PartitionSpec as P

HD = 128
BQ = 256
F32 = jnp.float32
BF16 = jnp.bfloat16
MESH = pl.DeviceIdType.MESH
NT = (((1,), (1,)), ((), ()))
NN = (((1,), (0,)), ((), ()))
TN = (((0,), (0,)), ((), ()))


def dot(a, b, dims):
    return lax.dot_general(a, b, dims, preferred_element_type=F32)


def feature(x):
    return jnp.where(x > 0, x + 1.0, jnp.exp(jnp.minimum(x, 0.0)))


def slope(x):
    return jnp.where(x > 0, 1.0, jnp.exp(jnp.minimum(x, 0.0)))


def split(x):
    high = x.astype(BF16)
    return high, (x - high.astype(F32)).astype(BF16)


def wide(x):
    return jnp.concatenate(split(x), axis=1)


def halves(y):
    return y[:, :HD] + y[:, HD:]


def sigmoid_row(x):
    return 1.0 / (1.0 + jnp.exp(-jnp.full((1, HD), x, F32)))


def cols(h):
    if isinstance(h, int):
        return pl.ds(h * HD, HD)
    return pl.ds(pl.multiple_of(h * HD, HD), HD)


def main_kernel(
    chips,
    heads,
    doc,
    gate,
    q_hbm,
    k_hbm,
    v_hbm,
    g_hbm,
    qg,
    kl,
    vl,
    later,
    small,
    q,
    k,
    v,
    g,
    qf,
    rden,
    part,
    gpart,
    mprev,
    npart,
    nprev,
    dpart,
    local_sum,
    stage,
    pair_f,
    pair_b,
    pair_n,
    pair_d,
    send1_f,
    recv1_f,
    send2_f,
    recv2_f,
    send1_b,
    recv1_b,
    send2_b,
    recv2_b,
    send_n,
    recv_n,
    send_d,
    recv_d,
    out_f,
    out_b,
    back_f,
    back_b,
    in_sems,
    send_sems,
    recv_sems,
):
    seq = lax.axis_index("seq")
    chip, core = seq // 2, seq % 2
    partner = seq + 1 - 2 * core
    rows = heads * HD
    half = rows // 2
    page = half // chips
    tokens = q.shape[0]
    blocks = tokens // BQ

    copies = [
        pltpu.make_async_copy(src, dst, in_sems.at[n])
        for n, (src, dst) in enumerate(((k_hbm, k), (v_hbm, v), (q_hbm, q), (g_hbm, g)))
    ]
    for c in copies:
        c.start()

    barrier = pltpu.get_barrier_semaphore()
    pl.semaphore_signal(barrier, inc=1, device_id={"seq": partner}, device_id_type=MESH)

    def greet(i, carry):
        peer = 2 * lax.rem(chip + 1 + i, chips) + core
        pl.semaphore_signal(barrier, inc=1, device_id={"seq": peer}, device_id_type=MESH)
        return carry

    lax.fori_loop(0, chips - 1, greet, 0)

    def linked(s):
        before = doc[jnp.maximum(s - 1, 0)]
        return jnp.where((s > 0) & (before == doc[s]), 1.0, 0.0)

    def linked_next(s):
        after = doc[jnp.minimum(s + 1, 2 * chips - 1)]
        return jnp.where((s < 2 * chips - 1) & (after == doc[s]), 1.0, 0.0)

    same_here = linked(2 * chip + 1)

    def to_partner(src, dst, n):
        return pltpu.make_async_remote_copy(
            src_ref=src,
            dst_ref=dst,
            send_sem=send_sems.at[n],
            recv_sem=recv_sems.at[n],
            device_id={"seq": partner},
            device_id_type=MESH,
        )

    def to_chips(source, dst, n):
        def push(i, carry):
            peer = lax.rem(chip + 1 + i, chips)
            pltpu.make_async_remote_copy(
                src_ref=source(peer),
                dst_ref=dst.at[chip],
                send_sem=send_sems.at[n],
                recv_sem=recv_sems.at[n],
                device_id={"seq": 2 * peer + core},
                device_id_type=MESH,
            ).start()
            return carry

        lax.fori_loop(0, chips - 1, push, 0)

    def all_pages(buffer, n):
        rest = buffer.at[pl.ds(0, chips - 1)]
        return pltpu.make_async_remote_copy(
            src_ref=rest,
            dst_ref=rest,
            send_sem=send_sems.at[n],
            recv_sem=recv_sems.at[n],
            device_id={"seq": partner},
            device_id_type=MESH,
        )

    own_rows = pl.ds(pl.multiple_of(core * half, 8), half)
    other_rows = pl.ds(pl.multiple_of((1 - core) * half, 8), half)

    plain_f = core == 0
    plain_b = core == 1

    def joined(plain, own, received):
        return jnp.where(plain, same_here, 1.0) * own + jnp.where(plain, 1.0, same_here) * received

    def chip_value(plain, mine, pair, stage_rows, send1, recv1, n):
        stage_rows[...] = joined(plain, mine[own_rows, :], pair[...])
        for j in range(chips):
            send1[j] = stage_rows[j * page : (j + 1) * page, :]
        recv1[chip] = send1[chip]
        to_chips(lambda peer: send1.at[peer], recv1, n)

    def forward_scan(recv1, send2, recv2, n):
        all_pages(recv1, n - 1).wait_recv()

        def step(t, run):
            before = linked(2 * t) * run
            send2[t] = before
            return recv1[t] + linked(2 * t + 1) * before

        lax.fori_loop(0, chips, step, jnp.zeros((page, HD), F32))
        recv2[chip] = send2[chip]
        to_chips(lambda peer: send2.at[peer], recv2, n)

    def backward_scan(recv1, send2, recv2, n):
        all_pages(recv1, n - 1).wait_recv()

        def step(i, run):
            t = chips - 1 - i
            after = linked_next(2 * t + 1) * run
            send2[t] = after
            return recv1[t] + linked_next(2 * t) * after

        lax.fori_loop(0, chips, step, jnp.zeros((page, HD), F32))
        recv2[chip] = send2[chip]
        to_chips(lambda peer: send2.at[peer], recv2, n)

    def hand_back(plain, mine, pair, recv2, stage_rows, out, full, back, n):
        all_pages(recv2, n - 1).wait_recv()
        for j in range(chips):
            stage_rows[j * page : (j + 1) * page, :] = recv2[j]
        chip_level = stage_rows[...]
        plain_part = jnp.where(plain, mine[own_rows, :], pair[...])
        added = same_here * (chip_level + plain_part)
        full[own_rows, :] = jnp.where(plain, chip_level, added)
        out[...] = jnp.where(plain, added, chip_level)
        to_partner(out, back, n).start()

    def take_back(full, out, back, n):
        to_partner(out, back, n).wait_recv()
        full[other_rows, :] = back[...]

    PN, PF, PB, PD = 0, 1, 2, 3
    BN, BD = 4, 5
    F1, F2, F3 = 6, 7, 8
    B1, B2, B3 = 9, 10, 11

    copies[0].wait()
    copies[1].wait()
    for h in range(heads):
        key_feature = feature(k[:, cols(h)].astype(F32)).astype(BF16)
        npart[h : h + 1, :] = jnp.sum(key_feature.astype(F32), axis=0, keepdims=True)
        part[h * HD : (h + 1) * HD, :] = dot(key_feature, v[:, cols(h)], TN)

    pl.semaphore_wait(barrier, chips)
    to_partner(npart, pair_n, PN).start()
    to_partner(part.at[other_rows], pair_f, PF).start()

    copies[2].wait()
    copies[3].wait()
    for h in range(heads):
        qf[:, cols(h)] = feature(q[:, cols(h)].astype(F32)).astype(BF16)

    to_partner(npart, pair_n, PN).wait_recv()
    send_n[...] = joined(plain_f, npart[...], pair_n[...])
    recv_n[chip] = send_n[...]
    to_chips(lambda peer: send_n, recv_n, BN)
    to_partner(part.at[other_rows], pair_f, PF).wait_recv()
    chip_value(plain_f, part, pair_f, stage, send1_f, recv1_f, F1)

    local_sum[...] = jnp.zeros_like(local_sum)

    def shares(h):
        share = sigmoid_row(gate[h])
        return share, 1.0 - share

    def attend(h, i):
        count = (i + 1) * BQ
        here = cols(h)
        queries = pl.ds(i * BQ, BQ)
        keys = pl.ds(0, count)
        local_share = shares(h)[1][:, :1]
        q_block, g_block = q[queries, here], g[queries, here]
        scores = dot(k[keys, here], q_block, NT) * (HD**-0.5 * math.log2(math.e))
        lead = scores[: count - BQ]
        last = scores[count - BQ :]
        key_ids = lax.broadcasted_iota(jnp.int32, (BQ, BQ), 0)
        query_ids = lax.broadcasted_iota(jnp.int32, (BQ, BQ), 1)
        last = jnp.where(key_ids <= query_ids, last, -1e30)
        scores = jnp.concatenate([lead, last], axis=0) if i else last
        weights = jnp.exp2(scores - jnp.max(scores, axis=0, keepdims=True))
        attention = weights * (1.0 / jnp.sum(weights, axis=0, keepdims=True))
        attention_low = attention.astype(BF16)
        value_dot = dot(v[keys, here], g_block, NT)
        delta = jnp.sum(value_dot * attention, axis=0, keepdims=True)
        score_grad = (attention * ((value_dot - delta) * local_share)).astype(BF16)
        seen = jnp.sum(value_dot * attention_low.astype(F32), axis=0, keepdims=True)
        local_sum[pl.ds(h, 1), :] += seen
        dk = dot(score_grad, q_block, NN)
        dv = dot(attention_low, g_block, NN)
        qg[queries, here] = dot(score_grad, k[keys, here], TN) * HD**-0.5
        if i == blocks - 1:
            kl[keys, here] = dk
            vl[keys, here] = dv
        else:
            kl[keys, here] += dk
            vl[keys, here] += dv

    def grad_to_memory():
        all_pages(recv_n, BN).wait_recv()
        own_doc = doc[2 * chip]

        def add(t, total):
            weight = jnp.where((t < chip) & (doc[2 * t + 1] == own_doc), 1.0, 0.0)
            return total + weight * recv_n[t]

        chip_level = lax.fori_loop(0, chips, add, jnp.zeros((heads, HD), F32))
        plain_part = jnp.where(plain_f, npart[...], pair_n[...])
        nprev[...] = jnp.where(plain_f, chip_level, same_here * (chip_level + plain_part))

        def one(h, carry):
            here = cols(h)
            share = shares(h)[0]
            high, low = split(jnp.broadcast_to(nprev[pl.ds(h, 1), :], (HD, HD)))
            features = qf[:, here]
            recip = 1.0 / (1.0 + (dot(features, high, NT) + dot(features, low, NT)))
            rden[:, here] = recip
            num_grad = g[:, here].astype(F32) * (share * recip)
            gpart[pl.ds(pl.multiple_of(h * HD, HD), HD), :] = halves(dot(features, wide(num_grad), TN))
            return carry

        lax.fori_loop(0, heads, one, 0)
        to_partner(gpart.at[other_rows], pair_b, PB).start()

    def read_memory():
        take_back(mprev, out_f, back_f, F3)
        lane = lax.broadcasted_iota(jnp.int32, (1, HD), 1)
        dpart[heads : heads + 1, :] = jnp.zeros((1, HD), F32)

        def one(h, carry):
            here = cols(h)
            share, local_share = shares(h)
            memory = mprev[pl.ds(pl.multiple_of(h * HD, HD), HD), :]
            features = qf[:, here]
            grads = g[:, here]
            recip = rden[:, here]
            memory_read = halves(dot(features, wide(memory), NN)) * recip
            row_sums = jnp.sum(grads.astype(F32) * memory_read, axis=1, keepdims=True)
            den_grad = -(row_sums * (share * recip))
            dpart[pl.ds(h, 1), :] = jnp.sum(features.astype(F32) * den_grad, axis=0, keepdims=True)
            read_sum = jnp.sum(row_sums, axis=0, keepdims=True)
            local_total = jnp.sum(local_sum[pl.ds(h, 1), :], axis=1, keepdims=True)
            gate_part = share * local_share * (read_sum - local_total)
            dpart[heads : heads + 1, :] += jnp.where(lane == h, gate_part, 0.0)
            high, low = split(memory)
            num_part = (dot(grads, high, NT) + dot(grads, low, NT)) * (share * recip)
            feature_grad = num_part + den_grad * nprev[pl.ds(h, 1), :]
            qg[:, here] += feature_grad * slope(q[:, here].astype(F32))
            return carry

        lax.fori_loop(0, heads, one, 0)
        to_partner(dpart, pair_d, PD).start()

    def spread_small():
        to_partner(dpart, pair_d, PD).wait_recv()
        send_d[0:heads, :] = joined(plain_b, dpart[0:heads, :], pair_d[0:heads, :])
        send_d[heads : heads + 1, :] = dpart[heads : heads + 1, :] + pair_d[heads : heads + 1, :]
        recv_d[chip] = send_d[...]
        to_chips(lambda peer: send_d, recv_d, BD)

    def gather_small():
        all_pages(recv_d, BD).wait_recv()
        own_doc = doc[2 * chip + 1]
        is_gate = lax.broadcasted_iota(jnp.int32, (heads + 1, HD), 0) == heads

        def add(t, total):
            weight = jnp.where((t > chip) & (doc[2 * t] == own_doc), 1.0, 0.0)
            return total + jnp.where(is_gate, 1.0, weight) * recv_d[t]

        total = lax.fori_loop(0, chips, add, jnp.zeros((heads + 1, HD), F32))
        plain_part = jnp.where(plain_b, dpart[...], pair_d[...])
        adjusted = jnp.where(plain_b, total, same_here * (total + plain_part))
        small[...] = jnp.where(is_gate, total, adjusted)

    def per_head(h, carry):
        attend(h, blocks - 1)

        @pl.when(h == 1)
        def _():
            to_partner(gpart.at[other_rows], pair_b, PB).wait_recv()
            chip_value(plain_b, gpart, pair_b, stage, send1_b, recv1_b, B1)
            forward_scan(recv1_f, send2_f, recv2_f, F2)

        @pl.when(h == 2)
        def _():
            backward_scan(recv1_b, send2_b, recv2_b, B2)

        for i in reversed(range(blocks - 1)):
            attend(h, i)

        @pl.when(h == 0)
        def _():
            grad_to_memory()

        return carry

    lax.fori_loop(0, heads, per_head, 0)

    hand_back(plain_f, part, pair_f, recv2_f, stage, out_f, mprev, back_f, F3)
    read_memory()
    spread_small()
    hand_back(plain_b, gpart, pair_b, recv2_b, stage, out_b, later, back_b, B3)
    take_back(later, out_b, back_b, B3)
    gather_small()

    for src, dst, n in (
        (npart, pair_n, PN),
        (part.at[other_rows], pair_f, PF),
        (gpart.at[other_rows], pair_b, PB),
        (dpart, pair_d, PD),
        (out_f, back_f, F3),
        (out_b, back_b, B3),
    ):
        to_partner(src, dst, n).wait_send()
    for buffer, n in (
        (recv_n, BN),
        (recv_d, BD),
        (recv1_f, F1),
        (recv2_f, F2),
        (recv1_b, B1),
        (recv2_b, B2),
    ):
        all_pages(buffer, n).wait_send()


def finish_kernel(heads, gate, later, small, k, v, qg, kl, vl, q_out, k_out, v_out, gate_out):
    q_out[...] = qg[...]
    for h in range(heads):
        here = cols(h)
        memory = later[h * HD : (h + 1) * HD, :]
        high, low = split(memory)
        keys = k[:, here].astype(F32)
        values = v[:, here]
        local_share = 1.0 - sigmoid_row(gate[h])
        grads = dot(values, high, NT) + dot(values, low, NT) + small[h : h + 1, :]
        k_out[:, here] = kl[:, here] * HD**-0.5 + grads * slope(keys)
        features = feature(keys).astype(BF16)
        v_out[:, here] = vl[:, here] * local_share + halves(dot(features, wide(memory), NN))
        gate_out[h] = small[heads, h]


def per_device(chips, queries, key_vectors, value_vectors, out_grad, gate_logit, doc_index):
    tokens, width = queries.shape
    heads = width // HD
    half = heads * HD // 2
    page = half // chips
    hbm = pl.BlockSpec(memory_space=pltpu.HBM)
    vmem = pl.BlockSpec(memory_space=pltpu.VMEM)
    smem = pl.BlockSpec(memory_space=pltpu.SMEM)
    local = jax.ShapeDtypeStruct((tokens, width), F32)
    state = jax.ShapeDtypeStruct((heads * HD, HD), F32)
    pages = pltpu.VMEM((chips, page, HD), F32)
    half_state = pltpu.VMEM((half, HD), F32)
    whole_state = pltpu.VMEM((heads * HD, HD), F32)
    operand = pltpu.VMEM((tokens, width), BF16)
    norms = pltpu.VMEM((heads, HD), F32)
    smalls = pltpu.VMEM((heads + 1, HD), F32)
    qg, kl, vl, later, small = pl.pallas_call(
        functools.partial(main_kernel, chips, heads),
        out_shape=(local, local, local, state, jax.ShapeDtypeStruct((heads + 1, HD), F32)),
        in_specs=[smem, smem, hbm, hbm, hbm, hbm],
        out_specs=[vmem] * 5,
        scratch_shapes=[
            operand,
            operand,
            operand,
            operand,
            operand,
            pltpu.VMEM((tokens, width), F32),
            whole_state,
            whole_state,
            whole_state,
            norms,
            norms,
            smalls,
            pltpu.VMEM((heads, BQ), F32),
            half_state,
            half_state,
            half_state,
            norms,
            smalls,
            pages,
            pages,
            pages,
            pages,
            pages,
            pages,
            pages,
            pages,
            norms,
            pltpu.VMEM((chips, heads, HD), F32),
            smalls,
            pltpu.VMEM((chips, heads + 1, HD), F32),
            half_state,
            half_state,
            half_state,
            half_state,
            pltpu.SemaphoreType.DMA((4,)),
            pltpu.SemaphoreType.DMA((12,)),
            pltpu.SemaphoreType.DMA((12,)),
        ],
        compiler_params=pltpu.CompilerParams(
            collective_id=0, has_side_effects=True, vmem_limit_bytes=36 * 1024 * 1024
        ),
        name="exchange",
    )(doc_index, gate_logit, queries, key_vectors, value_vectors, out_grad)

    block = pl.BlockSpec((BQ, width), lambda i: (i, 0))
    whole = pl.BlockSpec((heads * HD, HD), lambda i: (0, 0))
    return pl.pallas_call(
        functools.partial(finish_kernel, heads),
        grid=(tokens // BQ,),
        out_shape=(local, local, local, jax.ShapeDtypeStruct((heads,), F32)),
        in_specs=[
            smem,
            whole,
            pl.BlockSpec((heads + 1, HD), lambda i: (0, 0)),
            block,
            block,
            block,
            block,
            block,
        ],
        out_specs=[block, block, block, smem],
        compiler_params=pltpu.CompilerParams(vmem_limit_bytes=24 * 1024 * 1024),
        name="finish",
    )(gate_logit, later, small, key_vectors, value_vectors, qg, kl, vl)


def solution(mesh):
    spec = P("seq", "head")
    return jax.shard_map(
        functools.partial(per_device, mesh.shape["seq"] // 2),
        mesh=mesh,
        in_specs=(spec, spec, spec, spec, P("head"), P()),
        out_specs=(spec, spec, spec, P("head")),
        check_vma=False,
    )
```

```python
import functools
import math

import jax
import jax.numpy as jnp
from jax import lax
from jax.experimental import pallas as pl
from jax.experimental.pallas import tpu as pltpu
from jax.sharding import PartitionSpec as P

HD = 128
BQ = 256
F32 = jnp.float32
BF16 = jnp.bfloat16
MESH = pl.DeviceIdType.MESH
NT = (((1,), (1,)), ((), ()))
NN = (((1,), (0,)), ((), ()))
TN = (((0,), (0,)), ((), ()))


def dot(a, b, dims):
    return lax.dot_general(a, b, dims, preferred_element_type=F32)


def feature(x):
    return jnp.where(x > 0, x + 1.0, jnp.exp(jnp.minimum(x, 0.0)))


def slope(x):
    return jnp.where(x > 0, 1.0, jnp.exp(jnp.minimum(x, 0.0)))


def split(x):
    high = x.astype(BF16)
    return high, (x - high.astype(F32)).astype(BF16)


def wide(x):
    return jnp.concatenate(split(x), axis=1)


def halves(y):
    return y[:, :HD] + y[:, HD:]


def row_product(row, matrix):
    high, low = (jnp.broadcast_to(x, (16, x.shape[1])) for x in split(row))
    return (dot(high, matrix, NN) + dot(low, matrix, NN))[:1]


def flipped(x):
    return jnp.transpose(x)


def state_rows(h):
    return pl.ds(pl.multiple_of(h * HD, HD), HD)


def sigmoid_row(x):
    return 1.0 / (1.0 + jnp.exp(-jnp.full((1, HD), x, F32)))


def cols(h):
    if isinstance(h, int):
        return pl.ds(h * HD, HD)
    return pl.ds(pl.multiple_of(h * HD, HD), HD)


def main_kernel(
    chips,
    heads,
    doc,
    gate,
    q_hbm,
    k_hbm,
    v_hbm,
    g_hbm,
    qg,
    kl,
    vl,
    later,
    small,
    q,
    k,
    v,
    g,
    qf,
    qf_t,
    g_t,
    recip_rows,
    den_rows,
    part,
    gpart,
    mprev,
    npart,
    nprev,
    dpart,
    local_sum,
    stage,
    pair_f,
    pair_b,
    pair_n,
    pair_d,
    send1_f,
    recv1_f,
    send2_f,
    recv2_f,
    send1_b,
    recv1_b,
    send2_b,
    recv2_b,
    send_n,
    recv_n,
    send_d,
    recv_d,
    out_f,
    out_b,
    back_f,
    back_b,
    in_sems,
    send_sems,
    recv_sems,
):
    seq = lax.axis_index("seq")
    chip, core = seq // 2, seq % 2
    partner = seq + 1 - 2 * core
    rows = heads * HD
    half = rows // 2
    page = half // chips
    tokens = q.shape[0]
    blocks = tokens // BQ

    copies = [
        pltpu.make_async_copy(src, dst, in_sems.at[n])
        for n, (src, dst) in enumerate(((k_hbm, k), (v_hbm, v), (q_hbm, q), (g_hbm, g)))
    ]
    for c in copies:
        c.start()

    barrier = pltpu.get_barrier_semaphore()
    pl.semaphore_signal(barrier, inc=1, device_id={"seq": partner}, device_id_type=MESH)

    def greet(i, carry):
        peer = 2 * lax.rem(chip + 1 + i, chips) + core
        pl.semaphore_signal(barrier, inc=1, device_id={"seq": peer}, device_id_type=MESH)
        return carry

    lax.fori_loop(0, chips - 1, greet, 0)

    def linked(s):
        before = doc[jnp.maximum(s - 1, 0)]
        return jnp.where((s > 0) & (before == doc[s]), 1.0, 0.0)

    def linked_next(s):
        after = doc[jnp.minimum(s + 1, 2 * chips - 1)]
        return jnp.where((s < 2 * chips - 1) & (after == doc[s]), 1.0, 0.0)

    same_here = linked(2 * chip + 1)

    def to_partner(src, dst, n):
        return pltpu.make_async_remote_copy(
            src_ref=src,
            dst_ref=dst,
            send_sem=send_sems.at[n],
            recv_sem=recv_sems.at[n],
            device_id={"seq": partner},
            device_id_type=MESH,
        )

    def to_chips(source, dst, n):
        def push(i, carry):
            peer = lax.rem(chip + 1 + i, chips)
            pltpu.make_async_remote_copy(
                src_ref=source(peer),
                dst_ref=dst.at[chip],
                send_sem=send_sems.at[n],
                recv_sem=recv_sems.at[n],
                device_id={"seq": 2 * peer + core},
                device_id_type=MESH,
            ).start()
            return carry

        lax.fori_loop(0, chips - 1, push, 0)

    def all_pages(buffer, n):
        rest = buffer.at[pl.ds(0, chips - 1)]
        return pltpu.make_async_remote_copy(
            src_ref=rest,
            dst_ref=rest,
            send_sem=send_sems.at[n],
            recv_sem=recv_sems.at[n],
            device_id={"seq": partner},
            device_id_type=MESH,
        )

    own_rows = pl.ds(pl.multiple_of(core * half, 8), half)
    other_rows = pl.ds(pl.multiple_of((1 - core) * half, 8), half)

    plain_f = core == 0
    plain_b = core == 1

    def joined(plain, own, received):
        return jnp.where(plain, same_here, 1.0) * own + jnp.where(plain, 1.0, same_here) * received

    def chip_value(plain, mine, pair, stage_rows, send1, recv1, n):
        stage_rows[...] = joined(plain, mine[own_rows, :], pair[...])
        for j in range(chips):
            send1[j] = stage_rows[j * page : (j + 1) * page, :]
        recv1[chip] = send1[chip]
        to_chips(lambda peer: send1.at[peer], recv1, n)

    def forward_scan(recv1, send2, recv2, n):
        all_pages(recv1, n - 1).wait_recv()

        def step(t, run):
            before = linked(2 * t) * run
            send2[t] = before
            return recv1[t] + linked(2 * t + 1) * before

        lax.fori_loop(0, chips, step, jnp.zeros((page, HD), F32))
        recv2[chip] = send2[chip]
        to_chips(lambda peer: send2.at[peer], recv2, n)

    def backward_scan(recv1, send2, recv2, n):
        all_pages(recv1, n - 1).wait_recv()

        def step(i, run):
            t = chips - 1 - i
            after = linked_next(2 * t + 1) * run
            send2[t] = after
            return recv1[t] + linked_next(2 * t) * after

        lax.fori_loop(0, chips, step, jnp.zeros((page, HD), F32))
        recv2[chip] = send2[chip]
        to_chips(lambda peer: send2.at[peer], recv2, n)

    def hand_back(plain, mine, pair, recv2, stage_rows, out, full, back, n):
        all_pages(recv2, n - 1).wait_recv()
        for j in range(chips):
            stage_rows[j * page : (j + 1) * page, :] = recv2[j]
        chip_level = stage_rows[...]
        plain_part = jnp.where(plain, mine[own_rows, :], pair[...])
        added = same_here * (chip_level + plain_part)
        full[own_rows, :] = jnp.where(plain, chip_level, added)
        out[...] = jnp.where(plain, added, chip_level)
        to_partner(out, back, n).start()

    def take_back(full, out, back, n):
        to_partner(out, back, n).wait_recv()
        full[other_rows, :] = back[...]

    PN, PF, PB, PD = 0, 1, 2, 3
    BN, BD = 4, 5
    F1, F2, F3 = 6, 7, 8
    B1, B2, B3 = 9, 10, 11

    copies[0].wait()
    copies[1].wait()
    for h in range(heads):
        key_feature = feature(k[:, cols(h)].astype(F32)).astype(BF16)
        npart[h : h + 1, :] = jnp.sum(key_feature.astype(F32), axis=0, keepdims=True)
        part[h * HD : (h + 1) * HD, :] = dot(key_feature, v[:, cols(h)], TN)

    pl.semaphore_wait(barrier, chips)
    to_partner(npart, pair_n, PN).start()
    to_partner(part.at[other_rows], pair_f, PF).start()

    copies[2].wait()
    copies[3].wait()
    for h in range(heads):
        qf[:, cols(h)] = feature(q[:, cols(h)].astype(F32)).astype(BF16)

    to_partner(npart, pair_n, PN).wait_recv()
    send_n[...] = joined(plain_f, npart[...], pair_n[...])
    recv_n[chip] = send_n[...]
    to_chips(lambda peer: send_n, recv_n, BN)
    to_partner(part.at[other_rows], pair_f, PF).wait_recv()
    chip_value(plain_f, part, pair_f, stage, send1_f, recv1_f, F1)
    for h in range(heads):
        qf_t[h * HD : (h + 1) * HD, :] = flipped(qf[:, cols(h)])

    local_sum[...] = jnp.zeros_like(local_sum)

    def shares(h):
        share = sigmoid_row(gate[h])
        return share, 1.0 - share

    def attend(h, i):
        count = (i + 1) * BQ
        here = cols(h)
        queries = pl.ds(i * BQ, BQ)
        keys = pl.ds(0, count)
        local_share = shares(h)[1][:, :1]
        q_block, g_block = q[queries, here], g[queries, here]
        scores = dot(k[keys, here], q_block, NT) * (HD**-0.5 * math.log2(math.e))
        lead = scores[: count - BQ]
        last = scores[count - BQ :]
        key_ids = lax.broadcasted_iota(jnp.int32, (BQ, BQ), 0)
        query_ids = lax.broadcasted_iota(jnp.int32, (BQ, BQ), 1)
        last = jnp.where(key_ids <= query_ids, last, -1e30)
        scores = jnp.concatenate([lead, last], axis=0) if i else last
        weights = jnp.exp2(scores - jnp.max(scores, axis=0, keepdims=True))
        attention = weights * (1.0 / jnp.sum(weights, axis=0, keepdims=True))
        attention_low = attention.astype(BF16)
        value_dot = dot(v[keys, here], g_block, NT)
        delta = jnp.sum(value_dot * attention, axis=0, keepdims=True)
        score_grad = (attention * ((value_dot - delta) * local_share)).astype(BF16)
        seen = jnp.sum(value_dot * attention_low.astype(F32), axis=0, keepdims=True)
        local_sum[pl.ds(h, 1), :] += seen
        dk = dot(score_grad, q_block, NN)
        dv = dot(attention_low, g_block, NN)
        qg[queries, here] = dot(score_grad, k[keys, here], TN) * HD**-0.5
        if i == blocks - 1:
            kl[keys, here] = dk
            vl[keys, here] = dv
        else:
            kl[keys, here] += dk
            vl[keys, here] += dv

    def grad_to_memory():
        all_pages(recv_n, BN).wait_recv()
        own_doc = doc[2 * chip]

        def add(t, total):
            weight = jnp.where((t < chip) & (doc[2 * t + 1] == own_doc), 1.0, 0.0)
            return total + weight * recv_n[t]

        chip_level = lax.fori_loop(0, chips, add, jnp.zeros((heads, HD), F32))
        plain_part = jnp.where(plain_f, npart[...], pair_n[...])
        nprev[...] = jnp.where(plain_f, chip_level, same_here * (chip_level + plain_part))

        def one(n, carry):
            h = jnp.where(core == 0, heads - 1 - n, n)
            share = shares(h)[0][:, :1]
            features = qf_t[state_rows(h), :]
            recip = 1.0 / (1.0 + row_product(nprev[pl.ds(h, 1), :], features))
            recip_rows[pl.ds(h, 1), :] = recip
            high, low = split(features.astype(F32) * (share * recip))
            grads = g[:, cols(h)]
            gpart[state_rows(h), :] = dot(high, grads, NN) + dot(low, grads, NN)

            @pl.when(n == heads // 2)
            def _():
                to_partner(gpart.at[other_rows], pair_b, PB).start()

            return carry

        lax.fori_loop(0, heads, one, 0)

    def read_memory():
        lane = lax.broadcasted_iota(jnp.int32, (1, HD), 1)
        dpart[heads : heads + 1, :] = jnp.zeros((1, HD), F32)

        def one(h, carry):
            share, local_share = shares(h)
            high, low = split(mprev[state_rows(h), :])
            features = qf_t[state_rows(h), :]
            recip = recip_rows[pl.ds(h, 1), :]
            numerator = dot(high, features, TN) + dot(low, features, TN)
            products = g_t[state_rows(h), :].astype(F32) * numerator
            row_sums = jnp.sum(products, axis=0, keepdims=True) * recip
            den_grad = -(row_sums * (share[:, :1] * recip))
            den_rows[pl.ds(h, 1), :] = den_grad
            dpart[pl.ds(h, 1), :] = row_product(den_grad, qf[:, cols(h)])
            read_sum = jnp.sum(row_sums, axis=1, keepdims=True)
            local_total = jnp.sum(local_sum[pl.ds(h, 1), :], axis=1, keepdims=True)
            gate_part = share * local_share * (read_sum - local_total)
            dpart[heads : heads + 1, :] += jnp.where(lane == h, gate_part, 0.0)
            return carry

        lax.fori_loop(0, heads, one, 0)
        to_partner(dpart, pair_d, PD).start()

    def query_memory_grad():
        def one(h, carry):
            here = cols(h)
            high, low = split(mprev[state_rows(h), :])
            grads = g_t[state_rows(h), :]
            factor = shares(h)[0][:, :1] * recip_rows[pl.ds(h, 1), :]
            norm = jnp.transpose(jnp.broadcast_to(nprev[pl.ds(h, 1), :], (HD, HD)))[:, :1]
            feature_grad = (dot(high, grads, NN) + dot(low, grads, NN)) * factor
            feature_grad += norm * den_rows[pl.ds(h, 1), :]
            qg[:, here] += jnp.transpose(feature_grad) * slope(q[:, here].astype(F32))
            return carry

        lax.fori_loop(0, heads, one, 0)

    def spread_small():
        to_partner(dpart, pair_d, PD).wait_recv()
        send_d[0:heads, :] = joined(plain_b, dpart[0:heads, :], pair_d[0:heads, :])
        send_d[heads : heads + 1, :] = dpart[heads : heads + 1, :] + pair_d[heads : heads + 1, :]
        recv_d[chip] = send_d[...]
        to_chips(lambda peer: send_d, recv_d, BD)

    def gather_small():
        all_pages(recv_d, BD).wait_recv()
        own_doc = doc[2 * chip + 1]
        is_gate = lax.broadcasted_iota(jnp.int32, (heads + 1, HD), 0) == heads

        def add(t, total):
            weight = jnp.where((t > chip) & (doc[2 * t] == own_doc), 1.0, 0.0)
            return total + jnp.where(is_gate, 1.0, weight) * recv_d[t]

        total = lax.fori_loop(0, chips, add, jnp.zeros((heads + 1, HD), F32))
        plain_part = jnp.where(plain_b, dpart[...], pair_d[...])
        adjusted = jnp.where(plain_b, total, same_here * (total + plain_part))
        small[...] = jnp.where(is_gate, total, adjusted)

    def per_head(h, carry):
        for i in reversed(range(blocks)):
            attend(h, i)

        @pl.when(h == 0)
        def _():
            grad_to_memory()
            forward_scan(recv1_f, send2_f, recv2_f, F2)
            to_partner(gpart.at[other_rows], pair_b, PB).wait_recv()
            chip_value(plain_b, gpart, pair_b, stage, send1_b, recv1_b, B1)
            for n in range(heads):
                g_t[n * HD : (n + 1) * HD, :] = flipped(g[:, cols(n)])

        return carry

    lax.fori_loop(0, heads, per_head, 0)

    hand_back(plain_f, part, pair_f, recv2_f, stage, out_f, mprev, back_f, F3)
    backward_scan(recv1_b, send2_b, recv2_b, B2)
    take_back(mprev, out_f, back_f, F3)
    read_memory()
    spread_small()
    query_memory_grad()
    hand_back(plain_b, gpart, pair_b, recv2_b, stage, out_b, later, back_b, B3)
    gather_small()
    take_back(later, out_b, back_b, B3)

    for src, dst, n in (
        (npart, pair_n, PN),
        (part.at[other_rows], pair_f, PF),
        (gpart.at[other_rows], pair_b, PB),
        (dpart, pair_d, PD),
        (out_f, back_f, F3),
        (out_b, back_b, B3),
    ):
        to_partner(src, dst, n).wait_send()
    for buffer, n in (
        (recv_n, BN),
        (recv_d, BD),
        (recv1_f, F1),
        (recv2_f, F2),
        (recv1_b, B1),
        (recv2_b, B2),
    ):
        all_pages(buffer, n).wait_send()


def finish_kernel(
    heads, gate, later, small, k, v, qg, kl, vl, q_out, k_out, v_out, gate_out, k_rows, v_rows, sems
):
    blocks = k.shape[0] // BQ
    copies = [pltpu.make_async_copy(qg, q_out, sems.at[0])]
    copies[0].start()
    for i in range(blocks):
        rows = pl.ds(i * BQ, BQ)
        for h in range(heads):
            here = cols(h)
            memory = later[h * HD : (h + 1) * HD, :]
            high, low = split(memory)
            keys = k[rows, here].astype(F32)
            values = v[rows, here]
            local_share = 1.0 - sigmoid_row(gate[h])
            grads = dot(values, high, NT) + dot(values, low, NT) + small[h : h + 1, :]
            k_rows[rows, here] = kl[rows, here] * HD**-0.5 + grads * slope(keys)
            features = feature(keys).astype(BF16)
            v_rows[rows, here] = vl[rows, here] * local_share + halves(
                dot(features, wide(memory), NN)
            )
        for n, (buffer, out) in enumerate(((k_rows, k_out), (v_rows, v_out))):
            copy = pltpu.make_async_copy(buffer.at[rows], out.at[rows], sems.at[1 + 2 * i + n])
            copy.start()
            copies.append(copy)
    for h in range(heads):
        gate_out[h] = small[heads, h]
    for copy in copies:
        copy.wait()


def per_device(chips, queries, key_vectors, value_vectors, out_grad, gate_logit, doc_index):
    tokens, width = queries.shape
    heads = width // HD
    half = heads * HD // 2
    page = half // chips
    hbm = pl.BlockSpec(memory_space=pltpu.HBM)
    vmem = pl.BlockSpec(memory_space=pltpu.VMEM)
    smem = pl.BlockSpec(memory_space=pltpu.SMEM)
    local = jax.ShapeDtypeStruct((tokens, width), F32)
    state = jax.ShapeDtypeStruct((heads * HD, HD), F32)
    pages = pltpu.VMEM((chips, page, HD), F32)
    half_state = pltpu.VMEM((half, HD), F32)
    whole_state = pltpu.VMEM((heads * HD, HD), F32)
    operand = pltpu.VMEM((tokens, width), BF16)
    norms = pltpu.VMEM((heads, HD), F32)
    smalls = pltpu.VMEM((heads + 1, HD), F32)
    operands = (doc_index, gate_logit, queries, key_vectors, value_vectors, out_grad)
    qg, kl, vl, later, small = pl.pallas_call(
        functools.partial(main_kernel, chips, heads),
        out_shape=(local, local, local, state, jax.ShapeDtypeStruct((heads + 1, HD), F32)),
        in_specs=[smem, smem, hbm, hbm, hbm, hbm],
        out_specs=[vmem] * 5,
        scratch_shapes=[
            operand,
            operand,
            operand,
            operand,
            operand,
            pltpu.VMEM((width, tokens), BF16),
            pltpu.VMEM((width, tokens), BF16),
            pltpu.VMEM((heads, tokens), F32),
            pltpu.VMEM((heads, tokens), F32),
            whole_state,
            whole_state,
            whole_state,
            norms,
            norms,
            smalls,
            pltpu.VMEM((heads, BQ), F32),
            half_state,
            half_state,
            half_state,
            norms,
            smalls,
            pages,
            pages,
            pages,
            pages,
            pages,
            pages,
            pages,
            pages,
            norms,
            pltpu.VMEM((chips, heads, HD), F32),
            smalls,
            pltpu.VMEM((chips, heads + 1, HD), F32),
            half_state,
            half_state,
            half_state,
            half_state,
            pltpu.SemaphoreType.DMA((4,)),
            pltpu.SemaphoreType.DMA((12,)),
            pltpu.SemaphoreType.DMA((12,)),
        ],
        compiler_params=pltpu.CompilerParams(
            collective_id=0, has_side_effects=True, vmem_limit_bytes=36 * 1024 * 1024
        ),
        name="exchange",
    )(*(pltpu.with_memory_space_constraint(x, pltpu.HBM) for x in operands))

    return pl.pallas_call(
        functools.partial(finish_kernel, heads),
        out_shape=(local, local, local, jax.ShapeDtypeStruct((heads,), F32)),
        in_specs=[smem] + [vmem] * 7,
        out_specs=[hbm, hbm, hbm, smem],
        scratch_shapes=[
            pltpu.VMEM((tokens, width), F32),
            pltpu.VMEM((tokens, width), F32),
            pltpu.SemaphoreType.DMA((1 + 2 * (tokens // BQ),)),
        ],
        compiler_params=pltpu.CompilerParams(vmem_limit_bytes=24 * 1024 * 1024),
        name="finish",
    )(gate_logit, later, small, key_vectors, value_vectors, qg, kl, vl)


def solution(mesh):
    spec = P("seq", "head")
    return jax.shard_map(
        functools.partial(per_device, mesh.shape["seq"] // 2),
        mesh=mesh,
        in_specs=(spec, spec, spec, spec, P("head"), P()),
        out_specs=(spec, spec, spec, P("head")),
        check_vma=False,
    )
```

```python
import functools
import math

import jax
import jax.numpy as jnp
from jax import lax
from jax.experimental import pallas as pl
from jax.experimental.pallas import tpu as pltpu
from jax.sharding import PartitionSpec as P

HD = 128
BQ = 256
WIDE = 4
F32 = jnp.float32
BF16 = jnp.bfloat16
MESH = pl.DeviceIdType.MESH
NT = (((1,), (1,)), ((), ()))
NN = (((1,), (0,)), ((), ()))
TN = (((0,), (0,)), ((), ()))


def dot(a, b, dims):
    return lax.dot_general(a, b, dims, preferred_element_type=F32)


def feature(x):
    return jnp.where(x > 0, x + 1.0, jnp.exp(jnp.minimum(x, 0.0)))


def slope(x):
    return jnp.where(x > 0, 1.0, jnp.exp(jnp.minimum(x, 0.0)))


def split(x):
    high = x.astype(BF16)
    return high, (x - high.astype(F32)).astype(BF16)


def wide(x):
    return jnp.concatenate(split(x), axis=1)


def halves(y):
    return y[:, :HD] + y[:, HD:]


def row_product(row, matrix):
    high, low = (jnp.broadcast_to(x, (16, x.shape[1])) for x in split(row))
    return (dot(high, matrix, NN) + dot(low, matrix, NN))[:1]


def flipped(x):
    return jnp.transpose(x)


def state_rows(h):
    return pl.ds(pl.multiple_of(h * HD, HD), HD)


def sigmoid_row(x):
    return 1.0 / (1.0 + jnp.exp(-jnp.full((1, HD), x, F32)))


def cols(h):
    if isinstance(h, int):
        return pl.ds(h * HD, HD)
    return pl.ds(pl.multiple_of(h * HD, HD), HD)


def main_kernel(
    chips,
    heads,
    doc,
    gate,
    q_hbm,
    k_hbm,
    v_hbm,
    g_hbm,
    qg,
    kl,
    vl,
    later,
    small,
    q,
    k,
    v,
    g,
    qf,
    qf_t,
    g_t,
    recip_rows,
    den_rows,
    part,
    gpart,
    mprev,
    npart,
    nprev,
    dpart,
    local_sum,
    stage,
    pair_f,
    pair_b,
    pair_n,
    pair_d,
    send1_f,
    recv1_f,
    send2_f,
    recv2_f,
    send1_b,
    recv1_b,
    send2_b,
    recv2_b,
    send_n,
    recv_n,
    send_d,
    recv_d,
    out_f,
    out_b,
    back_f,
    back_b,
    in_sems,
    send_sems,
    recv_sems,
):
    seq = lax.axis_index("seq")
    chip, core = seq // 2, seq % 2
    partner = seq + 1 - 2 * core
    rows = heads * HD
    half = rows // 2
    page = half // chips
    tokens = q.shape[0]
    blocks = tokens // BQ

    copies = [
        pltpu.make_async_copy(src, dst, in_sems.at[n])
        for n, (src, dst) in enumerate(((k_hbm, k), (v_hbm, v), (q_hbm, q), (g_hbm, g)))
    ]
    for c in copies:
        c.start()

    deep = chips // WIDE
    peers = [
        lax.rem(chip // deep + a, WIDE) * deep + lax.rem(chip % deep + b, deep)
        for _, a, b in sorted(
            (-min(a, WIDE - a) - min(b, deep - b), a, b) for a in range(WIDE) for b in range(deep)
        )
        if a or b
    ]

    barrier = pltpu.get_barrier_semaphore()
    for peer in peers:
        there = {"seq": 2 * peer + core}
        pl.semaphore_signal(barrier, inc=1, device_id=there, device_id_type=MESH)
    pl.semaphore_signal(barrier, inc=1, device_id={"seq": partner}, device_id_type=MESH)

    def linked(s):
        before = doc[jnp.maximum(s - 1, 0)]
        return jnp.where((s > 0) & (before == doc[s]), 1.0, 0.0)

    def linked_next(s):
        after = doc[jnp.minimum(s + 1, 2 * chips - 1)]
        return jnp.where((s < 2 * chips - 1) & (after == doc[s]), 1.0, 0.0)

    same_here = linked(2 * chip + 1)

    def to_partner(src, dst, n):
        return pltpu.make_async_remote_copy(
            src_ref=src,
            dst_ref=dst,
            send_sem=send_sems.at[n],
            recv_sem=recv_sems.at[n],
            device_id={"seq": partner},
            device_id_type=MESH,
        )

    def to_chips(source, dst, n):
        for peer in peers:
            pltpu.make_async_remote_copy(
                src_ref=source(peer),
                dst_ref=dst.at[chip],
                send_sem=send_sems.at[n],
                recv_sem=recv_sems.at[n],
                device_id={"seq": 2 * peer + core},
                device_id_type=MESH,
            ).start()

    def all_pages(buffer, n):
        rest = buffer.at[pl.ds(0, chips - 1)]
        return pltpu.make_async_remote_copy(
            src_ref=rest,
            dst_ref=rest,
            send_sem=send_sems.at[n],
            recv_sem=recv_sems.at[n],
            device_id={"seq": partner},
            device_id_type=MESH,
        )

    own_rows = pl.ds(pl.multiple_of(core * half, 8), half)
    other_rows = pl.ds(pl.multiple_of((1 - core) * half, 8), half)

    plain_f = core == 0
    plain_b = core == 1

    def joined(plain, own, received):
        return jnp.where(plain, same_here, 1.0) * own + jnp.where(plain, 1.0, same_here) * received

    def chip_value(plain, mine, pair, stage_rows, send1, recv1, n):
        stage_rows[...] = joined(plain, mine[own_rows, :], pair[...])
        for j in range(chips):
            send1[j] = stage_rows[j * page : (j + 1) * page, :]
        recv1[chip] = send1[chip]
        to_chips(lambda peer: send1.at[peer], recv1, n)

    def forward_scan(recv1, send2, recv2, n):
        all_pages(recv1, n - 1).wait_recv()

        def step(t, run):
            before = linked(2 * t) * run
            send2[t] = before
            return recv1[t] + linked(2 * t + 1) * before

        lax.fori_loop(0, chips, step, jnp.zeros((page, HD), F32))
        recv2[chip] = send2[chip]
        to_chips(lambda peer: send2.at[peer], recv2, n)

    def backward_scan(recv1, send2, recv2, n):
        all_pages(recv1, n - 1).wait_recv()

        def step(i, run):
            t = chips - 1 - i
            after = linked_next(2 * t + 1) * run
            send2[t] = after
            return recv1[t] + linked_next(2 * t) * after

        lax.fori_loop(0, chips, step, jnp.zeros((page, HD), F32))
        recv2[chip] = send2[chip]
        to_chips(lambda peer: send2.at[peer], recv2, n)

    def hand_back(plain, mine, pair, recv2, stage_rows, out, full, back, n):
        all_pages(recv2, n - 1).wait_recv()
        for j in range(chips):
            stage_rows[j * page : (j + 1) * page, :] = recv2[j]
        chip_level = stage_rows[...]
        plain_part = jnp.where(plain, mine[own_rows, :], pair[...])
        added = same_here * (chip_level + plain_part)
        full[own_rows, :] = jnp.where(plain, chip_level, added)
        out[...] = jnp.where(plain, added, chip_level)
        to_partner(out, back, n).start()

    def take_back(full, out, back, n):
        to_partner(out, back, n).wait_recv()
        full[other_rows, :] = back[...]

    PN, PF, PB, PD = 0, 1, 2, 3
    BN, BD = 4, 5
    F1, F2, F3 = 6, 7, 8
    B1, B2, B3 = 9, 10, 11

    copies[0].wait()
    copies[1].wait()
    for h in range(heads):
        key_feature = feature(k[:, cols(h)].astype(F32)).astype(BF16)
        npart[h : h + 1, :] = jnp.sum(key_feature.astype(F32), axis=0, keepdims=True)
        part[h * HD : (h + 1) * HD, :] = dot(key_feature, v[:, cols(h)], TN)

    pl.semaphore_wait(barrier, chips)
    to_partner(npart, pair_n, PN).start()
    to_partner(part.at[other_rows], pair_f, PF).start()

    copies[2].wait()
    copies[3].wait()
    for h in range(heads):
        qf[:, cols(h)] = feature(q[:, cols(h)].astype(F32)).astype(BF16)

    to_partner(npart, pair_n, PN).wait_recv()
    send_n[...] = joined(plain_f, npart[...], pair_n[...])
    recv_n[chip] = send_n[...]
    to_chips(lambda peer: send_n, recv_n, BN)
    to_partner(part.at[other_rows], pair_f, PF).wait_recv()
    chip_value(plain_f, part, pair_f, stage, send1_f, recv1_f, F1)
    for h in range(heads):
        qf_t[h * HD : (h + 1) * HD, :] = flipped(qf[:, cols(h)])

    def shares(h):
        share = sigmoid_row(gate[h])
        return share, 1.0 - share

    def attend(h, i):
        count = (i + 1) * BQ
        here = cols(h)
        queries = pl.ds(i * BQ, BQ)
        keys = pl.ds(0, count)
        local_share = shares(h)[1][:, :1]
        q_block, g_block = q[queries, here], g[queries, here]
        scores = dot(k[keys, here], q_block, NT) * (HD**-0.5 * math.log2(math.e))
        lead = scores[: count - BQ]
        last = scores[count - BQ :]
        key_ids = lax.broadcasted_iota(jnp.int32, (BQ, BQ), 0)
        query_ids = lax.broadcasted_iota(jnp.int32, (BQ, BQ), 1)
        last = jnp.where(key_ids <= query_ids, last, -1e30)
        scores = jnp.concatenate([lead, last], axis=0) if i else last
        weights = jnp.exp2(scores - jnp.max(scores, axis=0, keepdims=True))
        attention = weights * (1.0 / jnp.sum(weights, axis=0, keepdims=True))
        attention_low = attention.astype(BF16)
        value_dot = dot(v[keys, here], g_block, NT)
        delta = jnp.sum(value_dot * attention, axis=0, keepdims=True)
        score_grad = (attention * ((value_dot - delta) * local_share)).astype(BF16)
        dk = dot(score_grad, q_block, NN)
        dv = dot(attention_low, g_block, NN)
        qg[queries, here] = dot(score_grad, k[keys, here], TN) * HD**-0.5
        if i == blocks - 1:
            kl[keys, here] = dk
            vl[keys, here] = dv
        else:
            kl[keys, here] += dk
            vl[keys, here] += dv

    def grad_to_memory():
        all_pages(recv_n, BN).wait_recv()
        own_doc = doc[2 * chip]

        def add(t, total):
            weight = jnp.where((t < chip) & (doc[2 * t + 1] == own_doc), 1.0, 0.0)
            return total + weight * recv_n[t]

        chip_level = lax.fori_loop(0, chips, add, jnp.zeros((heads, HD), F32))
        plain_part = jnp.where(plain_f, npart[...], pair_n[...])
        nprev[...] = jnp.where(plain_f, chip_level, same_here * (chip_level + plain_part))

        def one(n, carry):
            h = jnp.where(core == 0, heads - 1 - n, n)
            share = shares(h)[0][:, :1]
            features = qf_t[state_rows(h), :]
            recip = 1.0 / (1.0 + row_product(nprev[pl.ds(h, 1), :], features))
            recip_rows[pl.ds(h, 1), :] = recip
            high, low = split(features.astype(F32) * (share * recip))
            grads = g[:, cols(h)]
            gpart[state_rows(h), :] = dot(high, grads, NN) + dot(low, grads, NN)

            @pl.when(n == heads // 2)
            def _():
                to_partner(gpart.at[other_rows], pair_b, PB).start()

            return carry

        lax.fori_loop(0, heads, one, 0)

    def read_memory():
        lane = lax.broadcasted_iota(jnp.int32, (1, HD), 1)
        dpart[heads : heads + 1, :] = jnp.zeros((1, HD), F32)

        def one(h, carry):
            share, local_share = shares(h)
            high, low = split(mprev[state_rows(h), :])
            features = qf_t[state_rows(h), :]
            recip = recip_rows[pl.ds(h, 1), :]
            numerator = dot(high, features, TN) + dot(low, features, TN)
            products = g_t[state_rows(h), :].astype(F32) * numerator
            row_sums = jnp.sum(products, axis=0, keepdims=True) * recip
            den_grad = -(row_sums * (share[:, :1] * recip))
            den_rows[pl.ds(h, 1), :] = den_grad
            dpart[pl.ds(h, 1), :] = row_product(den_grad, qf[:, cols(h)])
            read_sum = jnp.sum(row_sums, axis=1, keepdims=True)
            local_total = jnp.sum(local_sum[pl.ds(h, 1), :], axis=1, keepdims=True)
            gate_part = share * local_share * (read_sum - local_total)
            dpart[heads : heads + 1, :] += jnp.where(lane == h, gate_part, 0.0)
            return carry

        lax.fori_loop(0, heads, one, 0)
        to_partner(dpart, pair_d, PD).start()

    def query_memory_grad():
        def one(h, carry):
            here = cols(h)
            high, low = split(mprev[state_rows(h), :])
            grads = g_t[state_rows(h), :]
            factor = shares(h)[0][:, :1] * recip_rows[pl.ds(h, 1), :]
            norm = jnp.transpose(jnp.broadcast_to(nprev[pl.ds(h, 1), :], (HD, HD)))[:, :1]
            feature_grad = (dot(high, grads, NN) + dot(low, grads, NN)) * factor
            feature_grad += norm * den_rows[pl.ds(h, 1), :]
            qg[:, here] += jnp.transpose(feature_grad) * slope(q[:, here].astype(F32))
            return carry

        lax.fori_loop(0, heads, one, 0)

    def spread_small():
        to_partner(dpart, pair_d, PD).wait_recv()
        send_d[0:heads, :] = joined(plain_b, dpart[0:heads, :], pair_d[0:heads, :])
        send_d[heads : heads + 1, :] = dpart[heads : heads + 1, :] + pair_d[heads : heads + 1, :]
        recv_d[chip] = send_d[...]
        to_chips(lambda peer: send_d, recv_d, BD)

    def gather_small():
        all_pages(recv_d, BD).wait_recv()
        own_doc = doc[2 * chip + 1]
        is_gate = lax.broadcasted_iota(jnp.int32, (heads + 1, HD), 0) == heads

        def add(t, total):
            weight = jnp.where((t > chip) & (doc[2 * t] == own_doc), 1.0, 0.0)
            return total + jnp.where(is_gate, 1.0, weight) * recv_d[t]

        total = lax.fori_loop(0, chips, add, jnp.zeros((heads + 1, HD), F32))
        plain_part = jnp.where(plain_b, dpart[...], pair_d[...])
        adjusted = jnp.where(plain_b, total, same_here * (total + plain_part))
        small[...] = jnp.where(is_gate, total, adjusted)

    def per_head(h, carry):
        for i in reversed(range(blocks)):
            attend(h, i)
        here = cols(h)
        local_sum[pl.ds(h, 1), :] = jnp.sum(v[:, here].astype(F32) * vl[:, here], axis=0, keepdims=True)

        @pl.when(h == 0)
        def _():
            grad_to_memory()
            forward_scan(recv1_f, send2_f, recv2_f, F2)
            to_partner(gpart.at[other_rows], pair_b, PB).wait_recv()
            chip_value(plain_b, gpart, pair_b, stage, send1_b, recv1_b, B1)
            for n in range(heads):
                g_t[n * HD : (n + 1) * HD, :] = flipped(g[:, cols(n)])

        return carry

    lax.fori_loop(0, heads, per_head, 0)

    hand_back(plain_f, part, pair_f, recv2_f, stage, out_f, mprev, back_f, F3)
    backward_scan(recv1_b, send2_b, recv2_b, B2)
    take_back(mprev, out_f, back_f, F3)
    read_memory()
    spread_small()
    query_memory_grad()
    hand_back(plain_b, gpart, pair_b, recv2_b, stage, out_b, later, back_b, B3)
    gather_small()
    take_back(later, out_b, back_b, B3)

    for src, dst, n in (
        (npart, pair_n, PN),
        (part.at[other_rows], pair_f, PF),
        (gpart.at[other_rows], pair_b, PB),
        (dpart, pair_d, PD),
        (out_f, back_f, F3),
        (out_b, back_b, B3),
    ):
        to_partner(src, dst, n).wait_send()
    for buffer, n in (
        (recv_n, BN),
        (recv_d, BD),
        (recv1_f, F1),
        (recv2_f, F2),
        (recv1_b, B1),
        (recv2_b, B2),
    ):
        all_pages(buffer, n).wait_send()


def finish_kernel(
    heads, gate, later, small, k, v, qg, kl, vl, q_out, k_out, v_out, gate_out, k_rows, v_rows, sems
):
    blocks = k.shape[0] // BQ
    copies = [pltpu.make_async_copy(qg, q_out, sems.at[0])]
    copies[0].start()
    for i in range(blocks):
        rows = pl.ds(i * BQ, BQ)
        for h in range(heads):
            here = cols(h)
            memory = later[h * HD : (h + 1) * HD, :]
            high, low = split(memory)
            keys = k[rows, here].astype(F32)
            values = v[rows, here]
            local_share = 1.0 - sigmoid_row(gate[h])
            grads = dot(values, high, NT) + dot(values, low, NT) + small[h : h + 1, :]
            k_rows[rows, here] = kl[rows, here] * HD**-0.5 + grads * slope(keys)
            features = feature(keys).astype(BF16)
            v_rows[rows, here] = vl[rows, here] * local_share + halves(
                dot(features, wide(memory), NN)
            )
        for n, (buffer, out) in enumerate(((k_rows, k_out), (v_rows, v_out))):
            copy = pltpu.make_async_copy(buffer.at[rows], out.at[rows], sems.at[1 + 2 * i + n])
            copy.start()
            copies.append(copy)
    for h in range(heads):
        gate_out[h] = small[heads, h]
    for copy in copies:
        copy.wait()


def per_device(chips, queries, key_vectors, value_vectors, out_grad, gate_logit, doc_index):
    tokens, width = queries.shape
    heads = width // HD
    half = heads * HD // 2
    page = half // chips
    hbm = pl.BlockSpec(memory_space=pltpu.HBM)
    vmem = pl.BlockSpec(memory_space=pltpu.VMEM)
    smem = pl.BlockSpec(memory_space=pltpu.SMEM)
    local = jax.ShapeDtypeStruct((tokens, width), F32)
    state = jax.ShapeDtypeStruct((heads * HD, HD), F32)
    pages = pltpu.VMEM((chips, page, HD), F32)
    half_state = pltpu.VMEM((half, HD), F32)
    whole_state = pltpu.VMEM((heads * HD, HD), F32)
    operand = pltpu.VMEM((tokens, width), BF16)
    norms = pltpu.VMEM((heads, HD), F32)
    smalls = pltpu.VMEM((heads + 1, HD), F32)
    operands = (doc_index, gate_logit, queries, key_vectors, value_vectors, out_grad)
    qg, kl, vl, later, small = pl.pallas_call(
        functools.partial(main_kernel, chips, heads),
        out_shape=(local, local, local, state, jax.ShapeDtypeStruct((heads + 1, HD), F32)),
        in_specs=[smem, smem, hbm, hbm, hbm, hbm],
        out_specs=[vmem] * 5,
        scratch_shapes=[
            operand,
            operand,
            operand,
            operand,
            operand,
            pltpu.VMEM((width, tokens), BF16),
            pltpu.VMEM((width, tokens), BF16),
            pltpu.VMEM((heads, tokens), F32),
            pltpu.VMEM((heads, tokens), F32),
            whole_state,
            whole_state,
            whole_state,
            norms,
            norms,
            smalls,
            pltpu.VMEM((heads, HD), F32),
            half_state,
            half_state,
            half_state,
            norms,
            smalls,
            pages,
            pages,
            pages,
            pages,
            pages,
            pages,
            pages,
            pages,
            norms,
            pltpu.VMEM((chips, heads, HD), F32),
            smalls,
            pltpu.VMEM((chips, heads + 1, HD), F32),
            half_state,
            half_state,
            half_state,
            half_state,
            pltpu.SemaphoreType.DMA((4,)),
            pltpu.SemaphoreType.DMA((12,)),
            pltpu.SemaphoreType.DMA((12,)),
        ],
        compiler_params=pltpu.CompilerParams(
            collective_id=0, has_side_effects=True, vmem_limit_bytes=36 * 1024 * 1024
        ),
        name="exchange",
    )(*(pltpu.with_memory_space_constraint(x, pltpu.HBM) for x in operands))

    return pl.pallas_call(
        functools.partial(finish_kernel, heads),
        out_shape=(local, local, local, jax.ShapeDtypeStruct((heads,), F32)),
        in_specs=[smem] + [vmem] * 7,
        out_specs=[hbm, hbm, hbm, smem],
        scratch_shapes=[
            pltpu.VMEM((tokens, width), F32),
            pltpu.VMEM((tokens, width), F32),
            pltpu.SemaphoreType.DMA((1 + 2 * (tokens // BQ),)),
        ],
        compiler_params=pltpu.CompilerParams(vmem_limit_bytes=24 * 1024 * 1024),
        name="finish",
    )(gate_logit, later, small, key_vectors, value_vectors, qg, kl, vl)


def solution(mesh):
    spec = P("seq", "head")
    return jax.shard_map(
        functools.partial(per_device, mesh.shape["seq"] // 2),
        mesh=mesh,
        in_specs=(spec, spec, spec, spec, P("head"), P()),
        out_specs=(spec, spec, spec, P("head")),
        check_vma=False,
    )
```

```python
import functools
import math

import jax
import jax.numpy as jnp
from jax import lax
from jax.experimental import pallas as pl
from jax.experimental.pallas import tpu as pltpu
from jax.sharding import PartitionSpec as P

HD = 128
BQ = 256
WIDE = 4
F32 = jnp.float32
BF16 = jnp.bfloat16
MESH = pl.DeviceIdType.MESH
NT = (((1,), (1,)), ((), ()))
NN = (((1,), (0,)), ((), ()))
TN = (((0,), (0,)), ((), ()))


def dot(a, b, dims):
    return lax.dot_general(a, b, dims, preferred_element_type=F32)


def feature(x):
    return jnp.where(x > 0, x + 1.0, jnp.exp(jnp.minimum(x, 0.0)))


def slope(x):
    return jnp.where(x > 0, 1.0, jnp.exp(jnp.minimum(x, 0.0)))


def split(x):
    high = x.astype(BF16)
    return high, (x - high.astype(F32)).astype(BF16)


def wide(x):
    return jnp.concatenate(split(x), axis=1)


def halves(y):
    return y[:, :HD] + y[:, HD:]


def row_product(row, matrix):
    high, low = (jnp.broadcast_to(x, (16, x.shape[1])) for x in split(row))
    return (dot(high, matrix, NN) + dot(low, matrix, NN))[:1]


def flipped(x):
    return jnp.transpose(x)


def state_rows(h):
    return pl.ds(pl.multiple_of(h * HD, HD), HD)


def sigmoid_row(x):
    return 1.0 / (1.0 + jnp.exp(-jnp.full((1, HD), x, F32)))


def cols(h):
    if isinstance(h, int):
        return pl.ds(h * HD, HD)
    return pl.ds(pl.multiple_of(h * HD, HD), HD)


def main_kernel(
    chips,
    heads,
    doc,
    gate,
    q_hbm,
    k_hbm,
    v_hbm,
    g_hbm,
    qg,
    kl,
    vl,
    later,
    small,
    q,
    k,
    v,
    g,
    qf,
    qf_t,
    g_t,
    recip_rows,
    den_rows,
    part,
    gpart,
    mprev,
    npart,
    nprev,
    dpart,
    local_sum,
    stage,
    pair_f,
    pair_b,
    pair_n,
    pair_d,
    send1_f,
    recv1_f,
    send2_f,
    recv2_f,
    send1_b,
    recv1_b,
    send2_b,
    recv2_b,
    send_n,
    recv_n,
    send_d,
    recv_d,
    out_f,
    out_b,
    back_f,
    back_b,
    in_sems,
    send_sems,
    recv_sems,
):
    seq = lax.axis_index("seq")
    chip, core = seq // 2, seq % 2
    partner = seq + 1 - 2 * core
    rows = heads * HD
    half = rows // 2
    page = half // chips
    tokens = q.shape[0]
    blocks = tokens // BQ

    copies = [
        pltpu.make_async_copy(src, dst, in_sems.at[n])
        for n, (src, dst) in enumerate(((k_hbm, k), (v_hbm, v), (q_hbm, q), (g_hbm, g)))
    ]
    for c in copies:
        c.start()

    deep = chips // WIDE
    peers = [
        lax.rem(chip // deep + a, WIDE) * deep + lax.rem(chip % deep + b, deep)
        for _, a, b in sorted(
            (-min(a, WIDE - a) - min(b, deep - b), a, b) for a in range(WIDE) for b in range(deep)
        )
        if a or b
    ]

    barrier = pltpu.get_barrier_semaphore()
    for peer in peers:
        there = {"seq": 2 * peer + core}
        pl.semaphore_signal(barrier, inc=1, device_id=there, device_id_type=MESH)
    pl.semaphore_signal(barrier, inc=1, device_id={"seq": partner}, device_id_type=MESH)

    def linked(s):
        before = doc[max(s - 1, 0) if isinstance(s, int) else jnp.maximum(s - 1, 0)]
        return jnp.where((s > 0) & (before == doc[s]), 1.0, 0.0)

    def linked_next(s):
        last = 2 * chips - 1
        after = doc[min(s + 1, last) if isinstance(s, int) else jnp.minimum(s + 1, last)]
        return jnp.where((s < last) & (after == doc[s]), 1.0, 0.0)

    same_here = linked(2 * chip + 1)

    def to_partner(src, dst, n):
        return pltpu.make_async_remote_copy(
            src_ref=src,
            dst_ref=dst,
            send_sem=send_sems.at[n],
            recv_sem=recv_sems.at[n],
            device_id={"seq": partner},
            device_id_type=MESH,
        )

    def to_chips(source, dst, n):
        for peer in peers:
            pltpu.make_async_remote_copy(
                src_ref=source(peer),
                dst_ref=dst.at[chip],
                send_sem=send_sems.at[n],
                recv_sem=recv_sems.at[n],
                device_id={"seq": 2 * peer + core},
                device_id_type=MESH,
            ).start()

    def all_pages(buffer, n):
        rest = buffer.at[pl.ds(0, chips - 1)]
        return pltpu.make_async_remote_copy(
            src_ref=rest,
            dst_ref=rest,
            send_sem=send_sems.at[n],
            recv_sem=recv_sems.at[n],
            device_id={"seq": partner},
            device_id_type=MESH,
        )

    own_rows = pl.ds(pl.multiple_of(core * half, 8), half)
    other_rows = pl.ds(pl.multiple_of((1 - core) * half, 8), half)

    plain_f = core == 0
    plain_b = core == 1

    def joined(plain, own, received):
        return jnp.where(plain, same_here, 1.0) * own + jnp.where(plain, 1.0, same_here) * received

    def chip_value(plain, mine, pair, stage_rows, send1, recv1, n):
        stage_rows[...] = joined(plain, mine[own_rows, :], pair[...])
        for j in range(chips):
            send1[j] = stage_rows[j * page : (j + 1) * page, :]
        recv1[chip] = send1[chip]
        to_chips(lambda peer: send1.at[peer], recv1, n)

    def forward_scan(recv1, send2, recv2, n):
        all_pages(recv1, n - 1).wait_recv()

        def step(t, run):
            before = linked(2 * t) * run
            send2[t] = before
            return recv1[t] + linked(2 * t + 1) * before

        run = jnp.zeros((page, HD), F32)
        for i in range(chips):
            run = step(i, run)
        recv2[chip] = send2[chip]
        to_chips(lambda peer: send2.at[peer], recv2, n)

    def backward_scan(recv1, send2, recv2, n):
        all_pages(recv1, n - 1).wait_recv()

        def step(i, run):
            t = chips - 1 - i
            after = linked_next(2 * t + 1) * run
            send2[t] = after
            return recv1[t] + linked_next(2 * t) * after

        run = jnp.zeros((page, HD), F32)
        for i in range(chips):
            run = step(i, run)
        recv2[chip] = send2[chip]
        to_chips(lambda peer: send2.at[peer], recv2, n)

    def hand_back(plain, mine, pair, recv2, stage_rows, out, full, back, n):
        all_pages(recv2, n - 1).wait_recv()
        for j in range(chips):
            stage_rows[j * page : (j + 1) * page, :] = recv2[j]
        chip_level = stage_rows[...]
        plain_part = jnp.where(plain, mine[own_rows, :], pair[...])
        added = same_here * (chip_level + plain_part)
        full[own_rows, :] = jnp.where(plain, chip_level, added)
        out[...] = jnp.where(plain, added, chip_level)
        to_partner(out, back, n).start()

    def take_back(full, out, back, n):
        to_partner(out, back, n).wait_recv()
        full[other_rows, :] = back[...]

    PN, PF, PB, PD = 0, 1, 2, 3
    BN, BD = 4, 5
    F1, F2, F3 = 6, 7, 8
    B1, B2, B3 = 9, 10, 11

    copies[0].wait()
    copies[1].wait()
    for h in range(heads):
        key_feature = feature(k[:, cols(h)].astype(F32)).astype(BF16)
        npart[h : h + 1, :] = jnp.sum(key_feature.astype(F32), axis=0, keepdims=True)
        part[h * HD : (h + 1) * HD, :] = dot(key_feature, v[:, cols(h)], TN)

    pl.semaphore_wait(barrier, chips)
    to_partner(npart, pair_n, PN).start()
    to_partner(part.at[other_rows], pair_f, PF).start()

    copies[2].wait()
    copies[3].wait()
    for h in range(heads):
        qf[:, cols(h)] = feature(q[:, cols(h)].astype(F32)).astype(BF16)

    to_partner(npart, pair_n, PN).wait_recv()
    send_n[...] = joined(plain_f, npart[...], pair_n[...])
    recv_n[chip] = send_n[...]
    to_chips(lambda peer: send_n, recv_n, BN)
    to_partner(part.at[other_rows], pair_f, PF).wait_recv()
    chip_value(plain_f, part, pair_f, stage, send1_f, recv1_f, F1)
    for h in range(heads):
        qf_t[h * HD : (h + 1) * HD, :] = flipped(qf[:, cols(h)])
        g_t[h * HD : (h + 1) * HD, :] = flipped(g[:, cols(h)])

    def shares(h):
        share = sigmoid_row(gate[h])
        return share, 1.0 - share

    def attend(h, i):
        count = (i + 1) * BQ
        here = cols(h)
        queries = pl.ds(i * BQ, BQ)
        keys = pl.ds(0, count)
        local_share = shares(h)[1][:, :1]
        q_block, g_block = q[queries, here], g[queries, here]
        scores = dot(k[keys, here], q_block, NT) * (HD**-0.5 * math.log2(math.e))
        lead = scores[: count - BQ]
        last = scores[count - BQ :]
        key_ids = lax.broadcasted_iota(jnp.int32, (BQ, BQ), 0)
        query_ids = lax.broadcasted_iota(jnp.int32, (BQ, BQ), 1)
        last = jnp.where(key_ids <= query_ids, last, -1e30)
        scores = jnp.concatenate([lead, last], axis=0) if i else last
        weights = jnp.exp2(scores - jnp.max(scores, axis=0, keepdims=True))
        attention = weights * (1.0 / jnp.sum(weights, axis=0, keepdims=True))
        attention_low = attention.astype(BF16)
        value_dot = dot(v[keys, here], g_block, NT)
        delta = jnp.sum(value_dot * attention, axis=0, keepdims=True)
        score_grad = (attention * ((value_dot - delta) * local_share)).astype(BF16)
        dk = dot(score_grad, q_block, NN)
        dv = dot(attention_low, g_block, NN)
        qg[queries, here] = dot(score_grad, k[keys, here], TN) * HD**-0.5
        if i == blocks - 1:
            kl[keys, here] = dk
            vl[keys, here] = dv
        else:
            kl[keys, here] += dk
            vl[keys, here] += dv

    def grad_to_memory():
        all_pages(recv_n, BN).wait_recv()
        own_doc = doc[2 * chip]

        def add(t, total):
            weight = jnp.where((t < chip) & (doc[2 * t + 1] == own_doc), 1.0, 0.0)
            return total + weight * recv_n[t]

        chip_level = jnp.zeros((heads, HD), F32)
        for t in range(chips):
            chip_level = add(t, chip_level)
        plain_part = jnp.where(plain_f, npart[...], pair_n[...])
        nprev[...] = jnp.where(plain_f, chip_level, same_here * (chip_level + plain_part))

        def one(n, carry):
            h = jnp.where(core == 0, heads - 1 - n, n)
            share = shares(h)[0][:, :1]
            features = qf_t[state_rows(h), :]
            recip = 1.0 / (1.0 + row_product(nprev[pl.ds(h, 1), :], features))
            recip_rows[pl.ds(h, 1), :] = recip
            high, low = split(features.astype(F32) * (share * recip))
            grads = g[:, cols(h)]
            gpart[state_rows(h), :] = dot(high, grads, NN) + dot(low, grads, NN)

            @pl.when(n == heads // 2)
            def _():
                to_partner(gpart.at[other_rows], pair_b, PB).start()

            return carry

        lax.fori_loop(0, heads, one, 0)

    def read_memory():
        lane = lax.broadcasted_iota(jnp.int32, (1, HD), 1)
        dpart[heads : heads + 1, :] = jnp.zeros((1, HD), F32)

        def one(n, carry):
            h = jnp.where(core == 0, n, heads - 1 - n)

            @pl.when(n == 1)
            def _():
                take_back(mprev, out_f, back_f, F3)

            share, local_share = shares(h)
            high, low = split(mprev[state_rows(h), :])
            features = qf_t[state_rows(h), :]
            recip = recip_rows[pl.ds(h, 1), :]
            numerator = dot(high, features, TN) + dot(low, features, TN)
            products = g_t[state_rows(h), :].astype(F32) * numerator
            row_sums = jnp.sum(products, axis=0, keepdims=True) * recip
            den_grad = -(row_sums * (share[:, :1] * recip))
            den_rows[pl.ds(h, 1), :] = den_grad
            dpart[pl.ds(h, 1), :] = row_product(den_grad, qf[:, cols(h)])
            read_sum = jnp.sum(row_sums, axis=1, keepdims=True)
            local_total = jnp.sum(local_sum[pl.ds(h, 1), :], axis=1, keepdims=True)
            gate_part = share * local_share * (read_sum - local_total)
            dpart[heads : heads + 1, :] += jnp.where(lane == h, gate_part, 0.0)
            return carry

        lax.fori_loop(0, heads, one, 0)
        to_partner(dpart, pair_d, PD).start()

    def query_memory_grad():
        def one(h, carry):
            here = cols(h)
            high, low = split(mprev[state_rows(h), :])
            grads = g_t[state_rows(h), :]
            factor = shares(h)[0][:, :1] * recip_rows[pl.ds(h, 1), :]
            norm = jnp.transpose(jnp.broadcast_to(nprev[pl.ds(h, 1), :], (HD, HD)))[:, :1]
            feature_grad = (dot(high, grads, NN) + dot(low, grads, NN)) * factor
            feature_grad += norm * den_rows[pl.ds(h, 1), :]
            qg[:, here] += jnp.transpose(feature_grad) * slope(q[:, here].astype(F32))
            return carry

        lax.fori_loop(0, heads, one, 0)

    def spread_small():
        to_partner(dpart, pair_d, PD).wait_recv()
        send_d[0:heads, :] = joined(plain_b, dpart[0:heads, :], pair_d[0:heads, :])
        send_d[heads : heads + 1, :] = dpart[heads : heads + 1, :] + pair_d[heads : heads + 1, :]
        recv_d[chip] = send_d[...]
        to_chips(lambda peer: send_d, recv_d, BD)

    def gather_small():
        all_pages(recv_d, BD).wait_recv()
        own_doc = doc[2 * chip + 1]
        is_gate = lax.broadcasted_iota(jnp.int32, (heads + 1, HD), 0) == heads

        def add(t, total):
            weight = jnp.where((t > chip) & (doc[2 * t] == own_doc), 1.0, 0.0)
            return total + jnp.where(is_gate, 1.0, weight) * recv_d[t]

        total = jnp.zeros((heads + 1, HD), F32)
        for t in range(chips):
            total = add(t, total)
        plain_part = jnp.where(plain_b, dpart[...], pair_d[...])
        adjusted = jnp.where(plain_b, total, same_here * (total + plain_part))
        small[...] = jnp.where(is_gate, total, adjusted)

    def per_head(h, carry):
        for i in reversed(range(blocks)):
            attend(h, i)
        here = cols(h)
        local_sum[pl.ds(h, 1), :] = jnp.sum(v[:, here].astype(F32) * vl[:, here], axis=0, keepdims=True)

        @pl.when(h == 0)
        def _():
            grad_to_memory()
            forward_scan(recv1_f, send2_f, recv2_f, F2)
            to_partner(gpart.at[other_rows], pair_b, PB).wait_recv()
            chip_value(plain_b, gpart, pair_b, stage, send1_b, recv1_b, B1)

        return carry

    lax.fori_loop(0, heads, per_head, 0)

    hand_back(plain_f, part, pair_f, recv2_f, stage, out_f, mprev, back_f, F3)
    backward_scan(recv1_b, send2_b, recv2_b, B2)
    read_memory()
    spread_small()
    query_memory_grad()
    hand_back(plain_b, gpart, pair_b, recv2_b, stage, out_b, later, back_b, B3)
    gather_small()
    take_back(later, out_b, back_b, B3)

    for src, dst, n in (
        (npart, pair_n, PN),
        (part.at[other_rows], pair_f, PF),
        (gpart.at[other_rows], pair_b, PB),
        (dpart, pair_d, PD),
        (out_f, back_f, F3),
        (out_b, back_b, B3),
    ):
        to_partner(src, dst, n).wait_send()
    for buffer, n in (
        (recv_n, BN),
        (recv_d, BD),
        (recv1_f, F1),
        (recv2_f, F2),
        (recv1_b, B1),
        (recv2_b, B2),
    ):
        all_pages(buffer, n).wait_send()


def finish_kernel(
    heads, gate, later, small, k, v, qg, kl, vl, q_out, k_out, v_out, gate_out, k_rows, v_rows, sems
):
    blocks = k.shape[0] // BQ
    copies = [pltpu.make_async_copy(qg, q_out, sems.at[0])]
    copies[0].start()
    for i in range(blocks):
        rows = pl.ds(i * BQ, BQ)
        for h in range(heads):
            here = cols(h)
            memory = later[h * HD : (h + 1) * HD, :]
            high, low = split(memory)
            keys = k[rows, here].astype(F32)
            values = v[rows, here]
            local_share = 1.0 - sigmoid_row(gate[h])
            grads = dot(values, high, NT) + dot(values, low, NT) + small[h : h + 1, :]
            k_rows[rows, here] = kl[rows, here] * HD**-0.5 + grads * slope(keys)
            features = feature(keys).astype(BF16)
            v_rows[rows, here] = vl[rows, here] * local_share + halves(
                dot(features, wide(memory), NN)
            )
        for n, (buffer, out) in enumerate(((k_rows, k_out), (v_rows, v_out))):
            copy = pltpu.make_async_copy(buffer.at[rows], out.at[rows], sems.at[1 + 2 * i + n])
            copy.start()
            copies.append(copy)
    for h in range(heads):
        gate_out[h] = small[heads, h]
    for copy in copies:
        copy.wait()


def per_device(chips, queries, key_vectors, value_vectors, out_grad, gate_logit, doc_index):
    tokens, width = queries.shape
    heads = width // HD
    half = heads * HD // 2
    page = half // chips
    hbm = pl.BlockSpec(memory_space=pltpu.HBM)
    vmem = pl.BlockSpec(memory_space=pltpu.VMEM)
    smem = pl.BlockSpec(memory_space=pltpu.SMEM)
    local = jax.ShapeDtypeStruct((tokens, width), F32)
    state = jax.ShapeDtypeStruct((heads * HD, HD), F32)
    pages = pltpu.VMEM((chips, page, HD), F32)
    half_state = pltpu.VMEM((half, HD), F32)
    whole_state = pltpu.VMEM((heads * HD, HD), F32)
    operand = pltpu.VMEM((tokens, width), BF16)
    norms = pltpu.VMEM((heads, HD), F32)
    smalls = pltpu.VMEM((heads + 1, HD), F32)
    operands = (doc_index, gate_logit, queries, key_vectors, value_vectors, out_grad)
    qg, kl, vl, later, small = pl.pallas_call(
        functools.partial(main_kernel, chips, heads),
        out_shape=(local, local, local, state, jax.ShapeDtypeStruct((heads + 1, HD), F32)),
        in_specs=[smem, smem, hbm, hbm, hbm, hbm],
        out_specs=[vmem] * 5,
        scratch_shapes=[
            operand,
            operand,
            operand,
            operand,
            operand,
            pltpu.VMEM((width, tokens), BF16),
            pltpu.VMEM((width, tokens), BF16),
            pltpu.VMEM((heads, tokens), F32),
            pltpu.VMEM((heads, tokens), F32),
            whole_state,
            whole_state,
            whole_state,
            norms,
            norms,
            smalls,
            pltpu.VMEM((heads, HD), F32),
            half_state,
            half_state,
            half_state,
            norms,
            smalls,
            pages,
            pages,
            pages,
            pages,
            pages,
            pages,
            pages,
            pages,
            norms,
            pltpu.VMEM((chips, heads, HD), F32),
            smalls,
            pltpu.VMEM((chips, heads + 1, HD), F32),
            half_state,
            half_state,
            half_state,
            half_state,
            pltpu.SemaphoreType.DMA((4,)),
            pltpu.SemaphoreType.DMA((12,)),
            pltpu.SemaphoreType.DMA((12,)),
        ],
        compiler_params=pltpu.CompilerParams(
            collective_id=0, has_side_effects=True, vmem_limit_bytes=36 * 1024 * 1024
        ),
        name="exchange",
    )(*(pltpu.with_memory_space_constraint(x, pltpu.HBM) for x in operands))

    return pl.pallas_call(
        functools.partial(finish_kernel, heads),
        out_shape=(local, local, local, jax.ShapeDtypeStruct((heads,), F32)),
        in_specs=[smem] + [vmem] * 7,
        out_specs=[hbm, hbm, hbm, smem],
        scratch_shapes=[
            pltpu.VMEM((tokens, width), F32),
            pltpu.VMEM((tokens, width), F32),
            pltpu.SemaphoreType.DMA((1 + 2 * (tokens // BQ),)),
        ],
        compiler_params=pltpu.CompilerParams(vmem_limit_bytes=24 * 1024 * 1024),
        name="finish",
    )(gate_logit, later, small, key_vectors, value_vectors, qg, kl, vl)


def solution(mesh):
    spec = P("seq", "head")
    return jax.shard_map(
        functools.partial(per_device, mesh.shape["seq"] // 2),
        mesh=mesh,
        in_specs=(spec, spec, spec, spec, P("head"), P()),
        out_specs=(spec, spec, spec, P("head")),
        check_vma=False,
    )
```

```python
import functools
import math

import jax
import jax.numpy as jnp
from jax import lax
from jax.experimental import pallas as pl
from jax.experimental.pallas import tpu as pltpu
from jax.sharding import PartitionSpec as P

HD = 128
BQ = 256
WIDE = 4
F32 = jnp.float32
BF16 = jnp.bfloat16
MESH = pl.DeviceIdType.MESH
NT = (((1,), (1,)), ((), ()))
NN = (((1,), (0,)), ((), ()))
TN = (((0,), (0,)), ((), ()))


def dot(a, b, dims):
    return lax.dot_general(a, b, dims, preferred_element_type=F32)


def feature(x):
    return jnp.where(x > 0, x + 1.0, jnp.exp(jnp.minimum(x, 0.0)))


def slope(x):
    return jnp.where(x > 0, 1.0, jnp.exp(jnp.minimum(x, 0.0)))


def split(x):
    high = x.astype(BF16)
    return high, (x - high.astype(F32)).astype(BF16)


def wide(x):
    return jnp.concatenate(split(x), axis=1)


def halves(y):
    return y[:, :HD] + y[:, HD:]


def row_product(row, matrix):
    high, low = (jnp.broadcast_to(x, (16, x.shape[1])) for x in split(row))
    return (dot(high, matrix, NN) + dot(low, matrix, NN))[:1]


def flipped(x):
    return jnp.transpose(x)


def state_rows(h):
    return pl.ds(pl.multiple_of(h * HD, HD), HD)


def sigmoid_row(x):
    return 1.0 / (1.0 + jnp.exp(-jnp.full((1, HD), x, F32)))


def cols(h):
    if isinstance(h, int):
        return pl.ds(h * HD, HD)
    return pl.ds(pl.multiple_of(h * HD, HD), HD)


def main_kernel(
    chips,
    heads,
    doc,
    gate,
    q_hbm,
    k_hbm,
    v_hbm,
    g_hbm,
    qg,
    kl,
    vl,
    later,
    small,
    q,
    k,
    v,
    g,
    qf,
    qf_t,
    g_t,
    recip_rows,
    den_rows,
    part,
    gpart,
    mprev,
    npart,
    nprev,
    dpart,
    local_sum,
    stage,
    pair_f,
    pair_b,
    pair_n,
    pair_d,
    send1_f,
    recv1_f,
    send2_f,
    recv2_f,
    send1_b,
    recv1_b,
    send2_b,
    recv2_b,
    send_n,
    recv_n,
    send_d,
    recv_d,
    out_f,
    out_b,
    back_f,
    back_b,
    in_sems,
    send_sems,
    recv_sems,
):
    seq = lax.axis_index("seq")
    chip, core = seq // 2, seq % 2
    partner = seq + 1 - 2 * core
    rows = heads * HD
    half = rows // 2
    page = half // chips
    tokens = q.shape[0]
    blocks = tokens // BQ

    copies = [
        pltpu.make_async_copy(src, dst, in_sems.at[n])
        for n, (src, dst) in enumerate(((k_hbm, k), (v_hbm, v), (q_hbm, q), (g_hbm, g)))
    ]
    for c in copies:
        c.start()

    deep = chips // WIDE
    peers = [
        lax.rem(chip // deep + a, WIDE) * deep + lax.rem(chip % deep + b, deep)
        for _, a, b in sorted(
            (-min(a, WIDE - a) - min(b, deep - b), a, b) for a in range(WIDE) for b in range(deep)
        )
        if a or b
    ]

    barrier = pltpu.get_barrier_semaphore()
    for peer in peers:
        there = {"seq": 2 * peer + core}
        pl.semaphore_signal(barrier, inc=1, device_id=there, device_id_type=MESH)
    pl.semaphore_signal(barrier, inc=1, device_id={"seq": partner}, device_id_type=MESH)

    def linked(s):
        before = doc[max(s - 1, 0) if isinstance(s, int) else jnp.maximum(s - 1, 0)]
        return jnp.where((s > 0) & (before == doc[s]), 1.0, 0.0)

    def linked_next(s):
        last = 2 * chips - 1
        after = doc[min(s + 1, last) if isinstance(s, int) else jnp.minimum(s + 1, last)]
        return jnp.where((s < last) & (after == doc[s]), 1.0, 0.0)

    same_here = linked(2 * chip + 1)

    def to_partner(src, dst, n):
        return pltpu.make_async_remote_copy(
            src_ref=src,
            dst_ref=dst,
            send_sem=send_sems.at[n],
            recv_sem=recv_sems.at[n],
            device_id={"seq": partner},
            device_id_type=MESH,
        )

    def to_chips(source, dst, n):
        for peer in peers:
            pltpu.make_async_remote_copy(
                src_ref=source(peer),
                dst_ref=dst.at[chip],
                send_sem=send_sems.at[n],
                recv_sem=recv_sems.at[n],
                device_id={"seq": 2 * peer + core},
                device_id_type=MESH,
            ).start()

    def all_pages(buffer, n):
        rest = buffer.at[pl.ds(0, chips - 1)]
        return pltpu.make_async_remote_copy(
            src_ref=rest,
            dst_ref=rest,
            send_sem=send_sems.at[n],
            recv_sem=recv_sems.at[n],
            device_id={"seq": partner},
            device_id_type=MESH,
        )

    own_rows = pl.ds(pl.multiple_of(core * half, 8), half)
    other_rows = pl.ds(pl.multiple_of((1 - core) * half, 8), half)

    plain_f = core == 0
    plain_b = core == 1

    def joined(plain, own, received):
        return jnp.where(plain, same_here, 1.0) * own + jnp.where(plain, 1.0, same_here) * received

    def chip_value(plain, mine, pair, stage_rows, send1, recv1, n):
        stage_rows[...] = joined(plain, mine[own_rows, :], pair[...])
        for j in range(chips):
            send1[j] = stage_rows[j * page : (j + 1) * page, :]
        recv1[chip] = send1[chip]
        to_chips(lambda peer: send1.at[peer], recv1, n)

    def forward_scan(recv1, send2, recv2, n):
        all_pages(recv1, n - 1).wait_recv()

        def step(t, run):
            before = linked(2 * t) * run
            send2[t] = before
            return recv1[t] + linked(2 * t + 1) * before

        run = jnp.zeros((page, HD), F32)
        for i in range(chips):
            run = step(i, run)
        recv2[chip] = send2[chip]
        to_chips(lambda peer: send2.at[peer], recv2, n)

    def backward_scan(recv1, send2, recv2, n):
        all_pages(recv1, n - 1).wait_recv()

        def step(i, run):
            t = chips - 1 - i
            after = linked_next(2 * t + 1) * run
            send2[t] = after
            return recv1[t] + linked_next(2 * t) * after

        run = jnp.zeros((page, HD), F32)
        for i in range(chips):
            run = step(i, run)
        recv2[chip] = send2[chip]
        to_chips(lambda peer: send2.at[peer], recv2, n)

    def hand_back(plain, mine, pair, recv2, stage_rows, out, full, back, n):
        all_pages(recv2, n - 1).wait_recv()
        for j in range(chips):
            stage_rows[j * page : (j + 1) * page, :] = recv2[j]
        chip_level = stage_rows[...]
        plain_part = jnp.where(plain, mine[own_rows, :], pair[...])
        added = same_here * (chip_level + plain_part)
        full[own_rows, :] = jnp.where(plain, chip_level, added)
        out[...] = jnp.where(plain, added, chip_level)
        to_partner(out, back, n).start()

    def take_back(full, out, back, n):
        to_partner(out, back, n).wait_recv()
        full[other_rows, :] = back[...]

    PN, PF, PB, PD = 0, 1, 2, 3
    BN, BD = 4, 5
    F1, F2, F3 = 6, 7, 8
    B1, B2, B3 = 9, 10, 11

    copies[0].wait()
    copies[1].wait()
    for h in range(heads):
        key_feature = feature(k[:, cols(h)].astype(F32)).astype(BF16)
        npart[h : h + 1, :] = jnp.sum(key_feature.astype(F32), axis=0, keepdims=True)
        part[h * HD : (h + 1) * HD, :] = dot(key_feature, v[:, cols(h)], TN)

    pl.semaphore_wait(barrier, chips)
    to_partner(npart, pair_n, PN).start()
    to_partner(part.at[other_rows], pair_f, PF).start()

    copies[2].wait()
    copies[3].wait()
    for h in range(heads):
        qf[:, cols(h)] = feature(q[:, cols(h)].astype(F32)).astype(BF16)

    to_partner(npart, pair_n, PN).wait_recv()
    send_n[...] = joined(plain_f, npart[...], pair_n[...])
    recv_n[chip] = send_n[...]
    to_chips(lambda peer: send_n, recv_n, BN)
    to_partner(part.at[other_rows], pair_f, PF).wait_recv()
    chip_value(plain_f, part, pair_f, stage, send1_f, recv1_f, F1)
    for h in range(heads):
        qf_t[h * HD : (h + 1) * HD, :] = flipped(qf[:, cols(h)])
        g_t[h * HD : (h + 1) * HD, :] = flipped(g[:, cols(h)])

    def shares(h):
        share = sigmoid_row(gate[h])
        return share, 1.0 - share

    def attend(h, i):
        count = (i + 1) * BQ
        here = cols(h)
        queries = pl.ds(i * BQ, BQ)
        keys = pl.ds(0, count)
        local_share = shares(h)[1][:, :1]
        q_block, g_block = q[queries, here], g[queries, here]
        scores = dot(k[keys, here], q_block, NT) * (HD**-0.5 * math.log2(math.e))
        lead = scores[: count - BQ]
        last = scores[count - BQ :]
        key_ids = lax.broadcasted_iota(jnp.int32, (BQ, BQ), 0)
        query_ids = lax.broadcasted_iota(jnp.int32, (BQ, BQ), 1)
        last = jnp.where(key_ids <= query_ids, last, -1e30)
        scores = jnp.concatenate([lead, last], axis=0) if i else last
        weights = jnp.exp2(scores - jnp.max(scores, axis=0, keepdims=True))
        attention = weights * (1.0 / jnp.sum(weights, axis=0, keepdims=True))
        attention_low = attention.astype(BF16)
        value_dot = dot(v[keys, here], g_block, NT)
        delta = jnp.sum(value_dot * attention, axis=0, keepdims=True)
        score_grad = (attention * ((value_dot - delta) * local_share)).astype(BF16)
        dk = dot(score_grad, q_block, NN)
        dv = dot(attention_low, g_block, NN)
        qg[queries, here] = dot(score_grad, k[keys, here], TN) * HD**-0.5
        if i == blocks - 1:
            kl[keys, here] = dk
            vl[keys, here] = dv
        else:
            kl[keys, here] += dk
            vl[keys, here] += dv

    def grad_to_memory():
        all_pages(recv_n, BN).wait_recv()
        own_doc = doc[2 * chip]

        def add(t, total):
            weight = jnp.where((t < chip) & (doc[2 * t + 1] == own_doc), 1.0, 0.0)
            return total + weight * recv_n[t]

        chip_level = jnp.zeros((heads, HD), F32)
        for t in range(chips):
            chip_level = add(t, chip_level)
        plain_part = jnp.where(plain_f, npart[...], pair_n[...])
        nprev[...] = jnp.where(plain_f, chip_level, same_here * (chip_level + plain_part))

        def one(n):
            h = jnp.where(core == 0, heads - 1 - n, n)
            share = shares(h)[0][:, :1]
            features = qf_t[state_rows(h), :]
            recip = 1.0 / (1.0 + row_product(nprev[pl.ds(h, 1), :], features))
            recip_rows[pl.ds(h, 1), :] = recip
            high, low = split(features.astype(F32) * (share * recip))
            grads = g[:, cols(h)]
            gpart[state_rows(h), :] = dot(high, grads, NN) + dot(low, grads, NN)

            if n == heads // 2:
                to_partner(gpart.at[other_rows], pair_b, PB).start()

        for n in range(heads):
            one(n)

    def read_memory():
        lane = lax.broadcasted_iota(jnp.int32, (1, HD), 1)
        dpart[heads : heads + 1, :] = jnp.zeros((1, HD), F32)

        def one(n):
            h = jnp.where(core == 0, n, heads - 1 - n)

            if n == 1:
                take_back(mprev, out_f, back_f, F3)

            share, local_share = shares(h)
            high, low = split(mprev[state_rows(h), :])
            features = qf_t[state_rows(h), :]
            recip = recip_rows[pl.ds(h, 1), :]
            numerator = dot(high, features, TN) + dot(low, features, TN)
            products = g_t[state_rows(h), :].astype(F32) * numerator
            row_sums = jnp.sum(products, axis=0, keepdims=True) * recip
            den_grad = -(row_sums * (share[:, :1] * recip))
            den_rows[pl.ds(h, 1), :] = den_grad
            dpart[pl.ds(h, 1), :] = row_product(den_grad, qf[:, cols(h)])
            read_sum = jnp.sum(row_sums, axis=1, keepdims=True)
            local_total = jnp.sum(local_sum[pl.ds(h, 1), :], axis=1, keepdims=True)
            gate_part = share * local_share * (read_sum - local_total)
            dpart[heads : heads + 1, :] += jnp.where(lane == h, gate_part, 0.0)
        for n in range(heads):
            one(n)
        to_partner(dpart, pair_d, PD).start()

    def query_memory_grad():
        def one(h):
            here = cols(h)
            high, low = split(mprev[state_rows(h), :])
            grads = g_t[state_rows(h), :]
            factor = shares(h)[0][:, :1] * recip_rows[pl.ds(h, 1), :]
            norm = jnp.transpose(jnp.broadcast_to(nprev[pl.ds(h, 1), :], (HD, HD)))[:, :1]
            feature_grad = (dot(high, grads, NN) + dot(low, grads, NN)) * factor
            feature_grad += norm * den_rows[pl.ds(h, 1), :]
            qg[:, here] += jnp.transpose(feature_grad) * slope(q[:, here].astype(F32))
        for n in range(heads):
            one(n)

    def spread_small():
        to_partner(dpart, pair_d, PD).wait_recv()
        send_d[0:heads, :] = joined(plain_b, dpart[0:heads, :], pair_d[0:heads, :])
        send_d[heads : heads + 1, :] = dpart[heads : heads + 1, :] + pair_d[heads : heads + 1, :]
        recv_d[chip] = send_d[...]
        to_chips(lambda peer: send_d, recv_d, BD)

    def gather_small():
        all_pages(recv_d, BD).wait_recv()
        own_doc = doc[2 * chip + 1]
        is_gate = lax.broadcasted_iota(jnp.int32, (heads + 1, HD), 0) == heads

        def add(t, total):
            weight = jnp.where((t > chip) & (doc[2 * t] == own_doc), 1.0, 0.0)
            return total + jnp.where(is_gate, 1.0, weight) * recv_d[t]

        total = jnp.zeros((heads + 1, HD), F32)
        for t in range(chips):
            total = add(t, total)
        plain_part = jnp.where(plain_b, dpart[...], pair_d[...])
        adjusted = jnp.where(plain_b, total, same_here * (total + plain_part))
        small[...] = jnp.where(is_gate, total, adjusted)

    def per_head(h, carry):
        for i in reversed(range(blocks)):
            attend(h, i)
        here = cols(h)
        local_sum[pl.ds(h, 1), :] = jnp.sum(v[:, here].astype(F32) * vl[:, here], axis=0, keepdims=True)

        @pl.when(h == 0)
        def _():
            grad_to_memory()
            forward_scan(recv1_f, send2_f, recv2_f, F2)
            to_partner(gpart.at[other_rows], pair_b, PB).wait_recv()
            chip_value(plain_b, gpart, pair_b, stage, send1_b, recv1_b, B1)

        return carry

    lax.fori_loop(0, heads, per_head, 0)

    hand_back(plain_f, part, pair_f, recv2_f, stage, out_f, mprev, back_f, F3)
    backward_scan(recv1_b, send2_b, recv2_b, B2)
    read_memory()
    spread_small()
    query_memory_grad()
    hand_back(plain_b, gpart, pair_b, recv2_b, stage, out_b, later, back_b, B3)
    gather_small()
    take_back(later, out_b, back_b, B3)

    for src, dst, n in (
        (npart, pair_n, PN),
        (part.at[other_rows], pair_f, PF),
        (gpart.at[other_rows], pair_b, PB),
        (dpart, pair_d, PD),
        (out_f, back_f, F3),
        (out_b, back_b, B3),
    ):
        to_partner(src, dst, n).wait_send()
    for buffer, n in (
        (recv_n, BN),
        (recv_d, BD),
        (recv1_f, F1),
        (recv2_f, F2),
        (recv1_b, B1),
        (recv2_b, B2),
    ):
        all_pages(buffer, n).wait_send()


def finish_kernel(
    heads, gate, later, small, k, v, qg, kl, vl, q_out, k_out, v_out, gate_out, k_rows, v_rows, sems
):
    blocks = k.shape[0] // BQ
    copies = [pltpu.make_async_copy(qg, q_out, sems.at[0])]
    copies[0].start()
    for i in range(blocks):
        rows = pl.ds(i * BQ, BQ)
        for h in range(heads):
            here = cols(h)
            memory = later[h * HD : (h + 1) * HD, :]
            high, low = split(memory)
            keys = k[rows, here].astype(F32)
            values = v[rows, here]
            local_share = 1.0 - sigmoid_row(gate[h])
            grads = dot(values, high, NT) + dot(values, low, NT) + small[h : h + 1, :]
            k_rows[rows, here] = kl[rows, here] * HD**-0.5 + grads * slope(keys)
            features = feature(keys).astype(BF16)
            v_rows[rows, here] = vl[rows, here] * local_share + halves(
                dot(features, wide(memory), NN)
            )
        for n, (buffer, out) in enumerate(((k_rows, k_out), (v_rows, v_out))):
            copy = pltpu.make_async_copy(buffer.at[rows], out.at[rows], sems.at[1 + 2 * i + n])
            copy.start()
            copies.append(copy)
    for h in range(heads):
        gate_out[h] = small[heads, h]
    for copy in copies:
        copy.wait()


def per_device(chips, queries, key_vectors, value_vectors, out_grad, gate_logit, doc_index):
    tokens, width = queries.shape
    heads = width // HD
    half = heads * HD // 2
    page = half // chips
    hbm = pl.BlockSpec(memory_space=pltpu.HBM)
    vmem = pl.BlockSpec(memory_space=pltpu.VMEM)
    smem = pl.BlockSpec(memory_space=pltpu.SMEM)
    local = jax.ShapeDtypeStruct((tokens, width), F32)
    state = jax.ShapeDtypeStruct((heads * HD, HD), F32)
    pages = pltpu.VMEM((chips, page, HD), F32)
    half_state = pltpu.VMEM((half, HD), F32)
    whole_state = pltpu.VMEM((heads * HD, HD), F32)
    operand = pltpu.VMEM((tokens, width), BF16)
    norms = pltpu.VMEM((heads, HD), F32)
    smalls = pltpu.VMEM((heads + 1, HD), F32)
    operands = (doc_index, gate_logit, queries, key_vectors, value_vectors, out_grad)
    qg, kl, vl, later, small = pl.pallas_call(
        functools.partial(main_kernel, chips, heads),
        out_shape=(local, local, local, state, jax.ShapeDtypeStruct((heads + 1, HD), F32)),
        in_specs=[smem, smem, hbm, hbm, hbm, hbm],
        out_specs=[vmem] * 5,
        scratch_shapes=[
            operand,
            operand,
            operand,
            operand,
            operand,
            pltpu.VMEM((width, tokens), BF16),
            pltpu.VMEM((width, tokens), BF16),
            pltpu.VMEM((heads, tokens), F32),
            pltpu.VMEM((heads, tokens), F32),
            whole_state,
            whole_state,
            whole_state,
            norms,
            norms,
            smalls,
            pltpu.VMEM((heads, HD), F32),
            half_state,
            half_state,
            half_state,
            norms,
            smalls,
            pages,
            pages,
            pages,
            pages,
            pages,
            pages,
            pages,
            pages,
            norms,
            pltpu.VMEM((chips, heads, HD), F32),
            smalls,
            pltpu.VMEM((chips, heads + 1, HD), F32),
            half_state,
            half_state,
            half_state,
            half_state,
            pltpu.SemaphoreType.DMA((4,)),
            pltpu.SemaphoreType.DMA((12,)),
            pltpu.SemaphoreType.DMA((12,)),
        ],
        compiler_params=pltpu.CompilerParams(
            collective_id=0, has_side_effects=True, vmem_limit_bytes=36 * 1024 * 1024
        ),
        name="exchange",
    )(*(pltpu.with_memory_space_constraint(x, pltpu.HBM) for x in operands))

    return pl.pallas_call(
        functools.partial(finish_kernel, heads),
        out_shape=(local, local, local, jax.ShapeDtypeStruct((heads,), F32)),
        in_specs=[smem] + [vmem] * 7,
        out_specs=[hbm, hbm, hbm, smem],
        scratch_shapes=[
            pltpu.VMEM((tokens, width), F32),
            pltpu.VMEM((tokens, width), F32),
            pltpu.SemaphoreType.DMA((1 + 2 * (tokens // BQ),)),
        ],
        compiler_params=pltpu.CompilerParams(vmem_limit_bytes=24 * 1024 * 1024),
        name="finish",
    )(gate_logit, later, small, key_vectors, value_vectors, qg, kl, vl)


def solution(mesh):
    spec = P("seq", "head")
    return jax.shard_map(
        functools.partial(per_device, mesh.shape["seq"] // 2),
        mesh=mesh,
        in_specs=(spec, spec, spec, spec, P("head"), P()),
        out_specs=(spec, spec, spec, P("head")),
        check_vma=False,
    )
```

```python
import functools
import math

import jax
import jax.numpy as jnp
from jax import lax
from jax.experimental import pallas as pl
from jax.experimental.pallas import tpu as pltpu
from jax.sharding import PartitionSpec as P

HD = 128
BQ = 256
OUT_ROWS = 128
WIDE = 4
F32 = jnp.float32
BF16 = jnp.bfloat16
MESH = pl.DeviceIdType.MESH
NT = (((1,), (1,)), ((), ()))
NN = (((1,), (0,)), ((), ()))
TN = (((0,), (0,)), ((), ()))


def dot(a, b, dims):
    return lax.dot_general(a, b, dims, preferred_element_type=F32)


def feature(x):
    return jnp.where(x > 0, x + 1.0, jnp.exp(jnp.minimum(x, 0.0)))


def slope(x):
    return jnp.where(x > 0, 1.0, jnp.exp(jnp.minimum(x, 0.0)))


def split(x):
    high = x.astype(BF16)
    return high, (x - high.astype(F32)).astype(BF16)


def wide(x):
    return jnp.concatenate(split(x), axis=1)


def halves(y):
    return y[:, :HD] + y[:, HD:]


def row_product(row, matrix):
    high, low = (jnp.broadcast_to(x, (16, x.shape[1])) for x in split(row))
    return (dot(high, matrix, NN) + dot(low, matrix, NN))[:1]


def flipped(x):
    return jnp.transpose(x)


def state_rows(h):
    return pl.ds(pl.multiple_of(h * HD, HD), HD)


def sigmoid_row(x):
    return 1.0 / (1.0 + jnp.exp(-jnp.full((1, HD), x, F32)))


def cols(h):
    if isinstance(h, int):
        return pl.ds(h * HD, HD)
    return pl.ds(pl.multiple_of(h * HD, HD), HD)


def main_kernel(
    chips,
    heads,
    doc,
    gate,
    q_hbm,
    k_hbm,
    v_hbm,
    g_hbm,
    qg,
    kl,
    vl,
    later,
    small,
    q,
    k,
    v,
    g,
    qf,
    qf_t,
    g_t,
    recip_rows,
    den_rows,
    part,
    gpart,
    mprev,
    npart,
    nprev,
    dpart,
    local_sum,
    stage,
    pair_f,
    pair_b,
    pair_n,
    pair_d,
    send1_f,
    recv1_f,
    send2_f,
    recv2_f,
    send1_b,
    recv1_b,
    send2_b,
    recv2_b,
    send_n,
    recv_n,
    send_d,
    recv_d,
    out_f,
    out_b,
    back_f,
    back_b,
    in_sems,
    send_sems,
    recv_sems,
):
    seq = lax.axis_index("seq")
    chip, core = seq // 2, seq % 2
    partner = seq + 1 - 2 * core
    rows = heads * HD
    half = rows // 2
    page = half // chips
    tokens = q.shape[0]
    blocks = tokens // BQ

    copies = [
        pltpu.make_async_copy(src, dst, in_sems.at[n])
        for n, (src, dst) in enumerate(((k_hbm, k), (v_hbm, v), (q_hbm, q), (g_hbm, g)))
    ]
    for c in copies:
        c.start()

    deep = chips // WIDE
    peers = [
        lax.rem(chip // deep + a, WIDE) * deep + lax.rem(chip % deep + b, deep)
        for _, a, b in sorted(
            (-min(a, WIDE - a) - min(b, deep - b), a, b) for a in range(WIDE) for b in range(deep)
        )
        if a or b
    ]

    barrier = pltpu.get_barrier_semaphore()
    for peer in peers:
        there = {"seq": 2 * peer + core}
        pl.semaphore_signal(barrier, inc=1, device_id=there, device_id_type=MESH)
    pl.semaphore_signal(barrier, inc=1, device_id={"seq": partner}, device_id_type=MESH)

    def linked(s):
        before = doc[max(s - 1, 0) if isinstance(s, int) else jnp.maximum(s - 1, 0)]
        return jnp.where((s > 0) & (before == doc[s]), 1.0, 0.0)

    def linked_next(s):
        last = 2 * chips - 1
        after = doc[min(s + 1, last) if isinstance(s, int) else jnp.minimum(s + 1, last)]
        return jnp.where((s < last) & (after == doc[s]), 1.0, 0.0)

    same_here = linked(2 * chip + 1)

    def to_partner(src, dst, n):
        return pltpu.make_async_remote_copy(
            src_ref=src,
            dst_ref=dst,
            send_sem=send_sems.at[n],
            recv_sem=recv_sems.at[n],
            device_id={"seq": partner},
            device_id_type=MESH,
        )

    def to_chips(source, dst, n):
        for peer in peers:
            pltpu.make_async_remote_copy(
                src_ref=source(peer),
                dst_ref=dst.at[chip],
                send_sem=send_sems.at[n],
                recv_sem=recv_sems.at[n],
                device_id={"seq": 2 * peer + core},
                device_id_type=MESH,
            ).start()

    def all_pages(buffer, n):
        rest = buffer.at[pl.ds(0, chips - 1)]
        return pltpu.make_async_remote_copy(
            src_ref=rest,
            dst_ref=rest,
            send_sem=send_sems.at[n],
            recv_sem=recv_sems.at[n],
            device_id={"seq": partner},
            device_id_type=MESH,
        )

    own_rows = pl.ds(pl.multiple_of(core * half, 8), half)
    other_rows = pl.ds(pl.multiple_of((1 - core) * half, 8), half)

    plain_f = core == 0
    plain_b = core == 1

    def joined(plain, own, received):
        return jnp.where(plain, same_here, 1.0) * own + jnp.where(plain, 1.0, same_here) * received

    def chip_value(plain, mine, pair, stage_rows, send1, recv1, n):
        stage_rows[...] = joined(plain, mine[own_rows, :], pair[...])
        for j in range(chips):
            send1[j] = stage_rows[j * page : (j + 1) * page, :]
        recv1[chip] = send1[chip]
        to_chips(lambda peer: send1.at[peer], recv1, n)

    def forward_scan(recv1, send2, recv2, n):
        all_pages(recv1, n - 1).wait_recv()

        def step(t, run):
            before = linked(2 * t) * run
            send2[t] = before
            return recv1[t] + linked(2 * t + 1) * before

        run = jnp.zeros((page, HD), F32)
        for i in range(chips):
            run = step(i, run)
        recv2[chip] = send2[chip]
        to_chips(lambda peer: send2.at[peer], recv2, n)

    def backward_scan(recv1, send2, recv2, n):
        all_pages(recv1, n - 1).wait_recv()

        def step(i, run):
            t = chips - 1 - i
            after = linked_next(2 * t + 1) * run
            send2[t] = after
            return recv1[t] + linked_next(2 * t) * after

        run = jnp.zeros((page, HD), F32)
        for i in range(chips):
            run = step(i, run)
        recv2[chip] = send2[chip]
        to_chips(lambda peer: send2.at[peer], recv2, n)

    def hand_back(plain, mine, pair, recv2, stage_rows, out, full, back, n):
        all_pages(recv2, n - 1).wait_recv()
        for j in range(chips):
            stage_rows[j * page : (j + 1) * page, :] = recv2[j]
        chip_level = stage_rows[...]
        plain_part = jnp.where(plain, mine[own_rows, :], pair[...])
        added = same_here * (chip_level + plain_part)
        full[own_rows, :] = jnp.where(plain, chip_level, added)
        out[...] = jnp.where(plain, added, chip_level)
        to_partner(out, back, n).start()

    def take_back(full, out, back, n):
        to_partner(out, back, n).wait_recv()
        full[other_rows, :] = back[...]

    PN, PF, PB, PD = 0, 1, 2, 3
    BN, BD = 4, 5
    F1, F2, F3 = 6, 7, 8
    B1, B2, B3 = 9, 10, 11

    copies[0].wait()
    copies[1].wait()
    for h in range(heads):
        key_feature = feature(k[:, cols(h)].astype(F32)).astype(BF16)
        npart[h : h + 1, :] = jnp.sum(key_feature.astype(F32), axis=0, keepdims=True)
        part[h * HD : (h + 1) * HD, :] = dot(key_feature, v[:, cols(h)], TN)

    pl.semaphore_wait(barrier, chips)
    to_partner(npart, pair_n, PN).start()
    to_partner(part.at[other_rows], pair_f, PF).start()

    copies[2].wait()
    copies[3].wait()
    for h in range(heads):
        qf[:, cols(h)] = feature(q[:, cols(h)].astype(F32)).astype(BF16)

    to_partner(npart, pair_n, PN).wait_recv()
    send_n[...] = joined(plain_f, npart[...], pair_n[...])
    recv_n[chip] = send_n[...]
    to_chips(lambda peer: send_n, recv_n, BN)
    to_partner(part.at[other_rows], pair_f, PF).wait_recv()
    chip_value(plain_f, part, pair_f, stage, send1_f, recv1_f, F1)
    for h in range(heads):
        qf_t[h * HD : (h + 1) * HD, :] = flipped(qf[:, cols(h)])
        g_t[h * HD : (h + 1) * HD, :] = flipped(g[:, cols(h)])

    def shares(h):
        share = sigmoid_row(gate[h])
        return share, 1.0 - share

    def attend(h, i):
        count = (i + 1) * BQ
        here = cols(h)
        queries = pl.ds(i * BQ, BQ)
        keys = pl.ds(0, count)
        local_share = shares(h)[1][:, :1]
        q_block, g_block = q[queries, here], g[queries, here]
        scores = dot(k[keys, here], q_block, NT) * (HD**-0.5 * math.log2(math.e))
        lead = scores[: count - BQ]
        last = scores[count - BQ :]
        key_ids = lax.broadcasted_iota(jnp.int32, (BQ, BQ), 0)
        query_ids = lax.broadcasted_iota(jnp.int32, (BQ, BQ), 1)
        last = jnp.where(key_ids <= query_ids, last, -1e30)
        scores = jnp.concatenate([lead, last], axis=0) if i else last
        weights = jnp.exp2(scores - jnp.max(scores, axis=0, keepdims=True))
        attention = weights * (1.0 / jnp.sum(weights, axis=0, keepdims=True))
        attention_low = attention.astype(BF16)
        value_dot = dot(v[keys, here], g_block, NT)
        delta = jnp.sum(value_dot * attention, axis=0, keepdims=True)
        score_grad = (attention * ((value_dot - delta) * local_share)).astype(BF16)
        dk = dot(score_grad, q_block, NN)
        dv = dot(attention_low, g_block, NN)
        qg[queries, here] = dot(score_grad, k[keys, here], TN) * HD**-0.5
        if i == blocks - 1:
            kl[keys, here] = dk
            vl[keys, here] = dv
        else:
            kl[keys, here] += dk
            vl[keys, here] += dv

    def grad_to_memory():
        all_pages(recv_n, BN).wait_recv()
        own_doc = doc[2 * chip]

        def add(t, total):
            weight = jnp.where((t < chip) & (doc[2 * t + 1] == own_doc), 1.0, 0.0)
            return total + weight * recv_n[t]

        chip_level = jnp.zeros((heads, HD), F32)
        for t in range(chips):
            chip_level = add(t, chip_level)
        plain_part = jnp.where(plain_f, npart[...], pair_n[...])
        nprev[...] = jnp.where(plain_f, chip_level, same_here * (chip_level + plain_part))

        def one(n):
            h = jnp.where(core == 0, heads - 1 - n, n)
            share = shares(h)[0][:, :1]
            features = qf_t[state_rows(h), :]
            recip = 1.0 / (1.0 + row_product(nprev[pl.ds(h, 1), :], features))
            recip_rows[pl.ds(h, 1), :] = recip
            high, low = split(features.astype(F32) * (share * recip))
            grads = g[:, cols(h)]
            gpart[state_rows(h), :] = dot(high, grads, NN) + dot(low, grads, NN)

            if n == heads // 2:
                to_partner(gpart.at[other_rows], pair_b, PB).start()

        for n in range(heads):
            one(n)

    def read_memory():
        lane = lax.broadcasted_iota(jnp.int32, (1, HD), 1)
        dpart[heads : heads + 1, :] = jnp.zeros((1, HD), F32)

        def one(n):
            h = jnp.where(core == 0, n, heads - 1 - n)

            if n == 1:
                take_back(mprev, out_f, back_f, F3)

            share, local_share = shares(h)
            high, low = split(mprev[state_rows(h), :])
            features = qf_t[state_rows(h), :]
            recip = recip_rows[pl.ds(h, 1), :]
            numerator = dot(high, features, TN) + dot(low, features, TN)
            products = g_t[state_rows(h), :].astype(F32) * numerator
            row_sums = jnp.sum(products, axis=0, keepdims=True) * recip
            den_grad = -(row_sums * (share[:, :1] * recip))
            den_rows[pl.ds(h, 1), :] = den_grad
            dpart[pl.ds(h, 1), :] = row_product(den_grad, qf[:, cols(h)])
            read_sum = jnp.sum(row_sums, axis=1, keepdims=True)
            local_total = jnp.sum(local_sum[pl.ds(h, 1), :], axis=1, keepdims=True)
            gate_part = share * local_share * (read_sum - local_total)
            dpart[heads : heads + 1, :] += jnp.where(lane == h, gate_part, 0.0)
        for n in range(heads):
            one(n)
        to_partner(dpart, pair_d, PD).start()

    def query_memory_grad():
        def one(h):
            here = cols(h)
            high, low = split(mprev[state_rows(h), :])
            grads = g_t[state_rows(h), :]
            factor = shares(h)[0][:, :1] * recip_rows[pl.ds(h, 1), :]
            norm = jnp.transpose(jnp.broadcast_to(nprev[pl.ds(h, 1), :], (HD, HD)))[:, :1]
            feature_grad = (dot(high, grads, NN) + dot(low, grads, NN)) * factor
            feature_grad += norm * den_rows[pl.ds(h, 1), :]
            qg[:, here] += jnp.transpose(feature_grad) * slope(q[:, here].astype(F32))
        for n in range(heads):
            one(n)

    def spread_small():
        to_partner(dpart, pair_d, PD).wait_recv()
        send_d[0:heads, :] = joined(plain_b, dpart[0:heads, :], pair_d[0:heads, :])
        send_d[heads : heads + 1, :] = dpart[heads : heads + 1, :] + pair_d[heads : heads + 1, :]
        recv_d[chip] = send_d[...]
        to_chips(lambda peer: send_d, recv_d, BD)

    def gather_small():
        all_pages(recv_d, BD).wait_recv()
        own_doc = doc[2 * chip + 1]
        is_gate = lax.broadcasted_iota(jnp.int32, (heads + 1, HD), 0) == heads

        def add(t, total):
            weight = jnp.where((t > chip) & (doc[2 * t] == own_doc), 1.0, 0.0)
            return total + jnp.where(is_gate, 1.0, weight) * recv_d[t]

        total = jnp.zeros((heads + 1, HD), F32)
        for t in range(chips):
            total = add(t, total)
        plain_part = jnp.where(plain_b, dpart[...], pair_d[...])
        adjusted = jnp.where(plain_b, total, same_here * (total + plain_part))
        small[...] = jnp.where(is_gate, total, adjusted)

    def per_head(h, carry):
        for i in reversed(range(blocks)):
            attend(h, i)
        here = cols(h)
        local_sum[pl.ds(h, 1), :] = jnp.sum(v[:, here].astype(F32) * vl[:, here], axis=0, keepdims=True)

        @pl.when(h == 0)
        def _():
            grad_to_memory()
            forward_scan(recv1_f, send2_f, recv2_f, F2)
            to_partner(gpart.at[other_rows], pair_b, PB).wait_recv()
            chip_value(plain_b, gpart, pair_b, stage, send1_b, recv1_b, B1)

        return carry

    lax.fori_loop(0, heads, per_head, 0)

    hand_back(plain_f, part, pair_f, recv2_f, stage, out_f, mprev, back_f, F3)
    backward_scan(recv1_b, send2_b, recv2_b, B2)
    read_memory()
    spread_small()
    query_memory_grad()
    hand_back(plain_b, gpart, pair_b, recv2_b, stage, out_b, later, back_b, B3)
    gather_small()
    take_back(later, out_b, back_b, B3)

    for src, dst, n in (
        (npart, pair_n, PN),
        (part.at[other_rows], pair_f, PF),
        (gpart.at[other_rows], pair_b, PB),
        (dpart, pair_d, PD),
        (out_f, back_f, F3),
        (out_b, back_b, B3),
    ):
        to_partner(src, dst, n).wait_send()
    for buffer, n in (
        (recv_n, BN),
        (recv_d, BD),
        (recv1_f, F1),
        (recv2_f, F2),
        (recv1_b, B1),
        (recv2_b, B2),
    ):
        all_pages(buffer, n).wait_send()


def finish_kernel(
    heads, gate, later, small, k, v, qg, kl, vl, q_out, k_out, v_out, gate_out, k_rows, v_rows, sems
):
    blocks = k.shape[0] // OUT_ROWS
    copies = [pltpu.make_async_copy(qg, q_out, sems.at[0])]
    copies[0].start()
    for i in range(blocks):
        rows = pl.ds(i * OUT_ROWS, OUT_ROWS)
        for h in range(heads):
            here = cols(h)
            memory = later[h * HD : (h + 1) * HD, :]
            high, low = split(memory)
            keys = k[rows, here].astype(F32)
            values = v[rows, here]
            local_share = 1.0 - sigmoid_row(gate[h])
            grads = dot(values, high, NT) + dot(values, low, NT) + small[h : h + 1, :]
            k_rows[rows, here] = kl[rows, here] * HD**-0.5 + grads * slope(keys)
            features = feature(keys).astype(BF16)
            v_rows[rows, here] = vl[rows, here] * local_share + halves(
                dot(features, wide(memory), NN)
            )
        for n, (buffer, out) in enumerate(((k_rows, k_out), (v_rows, v_out))):
            copy = pltpu.make_async_copy(buffer.at[rows], out.at[rows], sems.at[1 + 2 * i + n])
            copy.start()
            copies.append(copy)
    for h in range(heads):
        gate_out[h] = small[heads, h]
    for copy in copies:
        copy.wait()


def per_device(chips, queries, key_vectors, value_vectors, out_grad, gate_logit, doc_index):
    tokens, width = queries.shape
    heads = width // HD
    half = heads * HD // 2
    page = half // chips
    hbm = pl.BlockSpec(memory_space=pltpu.HBM)
    vmem = pl.BlockSpec(memory_space=pltpu.VMEM)
    smem = pl.BlockSpec(memory_space=pltpu.SMEM)
    local = jax.ShapeDtypeStruct((tokens, width), F32)
    state = jax.ShapeDtypeStruct((heads * HD, HD), F32)
    pages = pltpu.VMEM((chips, page, HD), F32)
    half_state = pltpu.VMEM((half, HD), F32)
    whole_state = pltpu.VMEM((heads * HD, HD), F32)
    operand = pltpu.VMEM((tokens, width), BF16)
    norms = pltpu.VMEM((heads, HD), F32)
    smalls = pltpu.VMEM((heads + 1, HD), F32)
    operands = (doc_index, gate_logit, queries, key_vectors, value_vectors, out_grad)
    qg, kl, vl, later, small = pl.pallas_call(
        functools.partial(main_kernel, chips, heads),
        out_shape=(local, local, local, state, jax.ShapeDtypeStruct((heads + 1, HD), F32)),
        in_specs=[smem, smem, hbm, hbm, hbm, hbm],
        out_specs=[vmem] * 5,
        scratch_shapes=[
            operand,
            operand,
            operand,
            operand,
            operand,
            pltpu.VMEM((width, tokens), BF16),
            pltpu.VMEM((width, tokens), BF16),
            pltpu.VMEM((heads, tokens), F32),
            pltpu.VMEM((heads, tokens), F32),
            whole_state,
            whole_state,
            whole_state,
            norms,
            norms,
            smalls,
            pltpu.VMEM((heads, HD), F32),
            half_state,
            half_state,
            half_state,
            norms,
            smalls,
            pages,
            pages,
            pages,
            pages,
            pages,
            pages,
            pages,
            pages,
            norms,
            pltpu.VMEM((chips, heads, HD), F32),
            smalls,
            pltpu.VMEM((chips, heads + 1, HD), F32),
            half_state,
            half_state,
            half_state,
            half_state,
            pltpu.SemaphoreType.DMA((4,)),
            pltpu.SemaphoreType.DMA((12,)),
            pltpu.SemaphoreType.DMA((12,)),
        ],
        compiler_params=pltpu.CompilerParams(
            collective_id=0, has_side_effects=True, vmem_limit_bytes=36 * 1024 * 1024
        ),
        name="exchange",
    )(*(pltpu.with_memory_space_constraint(x, pltpu.HBM) for x in operands))

    return pl.pallas_call(
        functools.partial(finish_kernel, heads),
        out_shape=(local, local, local, jax.ShapeDtypeStruct((heads,), F32)),
        in_specs=[smem] + [vmem] * 7,
        out_specs=[hbm, hbm, hbm, smem],
        scratch_shapes=[
            pltpu.VMEM((tokens, width), F32),
            pltpu.VMEM((tokens, width), F32),
            pltpu.SemaphoreType.DMA((1 + 2 * (tokens // OUT_ROWS),)),
        ],
        compiler_params=pltpu.CompilerParams(vmem_limit_bytes=24 * 1024 * 1024),
        name="finish",
    )(gate_logit, later, small, key_vectors, value_vectors, qg, kl, vl)


def solution(mesh):
    spec = P("seq", "head")
    return jax.shard_map(
        functools.partial(per_device, mesh.shape["seq"] // 2),
        mesh=mesh,
        in_specs=(spec, spec, spec, spec, P("head"), P()),
        out_specs=(spec, spec, spec, P("head")),
        check_vma=False,
    )
```
